128 devices in a mesh: clip: 8 (over z, core), tm: 16 (over y, x).
Axes of the slice: x: 4, y: 4, z: 4, core: 2. Of those that a mesh axis runs over, the one named last changes fastest.
Arguments:
- tokens: bfloat16 [8, 16, 256, 2048], P('clip', 'tm'), may hold values from -16 to 16
- spatial_queries: bfloat16 [8, 16, 256, 1024], P('clip', 'tm'), may hold values from -4.5 to 4.5
- spatial_keys: bfloat16 [8, 16, 256, 1024], P('clip', 'tm'), may hold values from -4.5 to 4.5
- spatial_values: bfloat16 [8, 16, 256, 1024], P('clip', 'tm'), may hold values from -6 to 6
- spatial_proj: bfloat16 [1024, 2048], P('tm'), may hold values from -0.1875 to 0.1875
- temporal_qkv: bfloat16 [2048, 3072], P('tm'), may hold values from -0.13258252 to 0.13258252
- temporal_proj: bfloat16 [1024, 2048], P('tm'), may hold values from -0.1875 to 0.1875
- frame_mask: int32 [8, 16, 16], P('clip'), may hold values from 0 to 1, as said below
- expert_ids: int32 [8, 16, 256, 2], P('clip', 'tm'), may hold values from 0 to 127, all different within a row; in each aligned block of 256 rows (0 to 255, 256 to 511, ..., all dimensions but the last counted through in order) at most 8 rows name the same one
- gate_values: float32 [8, 16, 256, 2], P('clip', 'tm'), may hold values from 0.2 to 1
- expert_gate: bfloat16 [128, 2048, 1408], P(('clip', 'tm')), may hold values from -0.125 to 0.125
- expert_up: bfloat16 [128, 2048, 1408], P(('clip', 'tm')), may hold values from -0.125 to 0.125
- expert_down: bfloat16 [128, 1408, 2048], P(('clip', 'tm')), may hold values from -0.15625 to 0.15625
Outputs:
- layer_out: bfloat16 [8, 16, 256, 2048], P('clip', 'tm')
The draws below stay inside these ranges and needn't reach their ends.
Inputs may be any that keep to these rules, and one draw needn't show every extreme that they name: `expert_ids`: each token names 2 different experts. Among the 256 tokens of one clip and frame, no expert is named by more than 8 tokens, and in some frames one expert is named by exactly 8. frame_mask[c, i, j] is 1 where j = i and 0 where j > i.
All inputs are finite; a program needn't handle non-finite values.
Results may differ from the reference program's by a relative error of at most 0.013.
Values may be sent and summed in bfloat16 or wider, within the bound.
A program may use at most 128 MiB of HBM per device.

```python
import math
import jax
import jax.numpy as jnp
import numpy as np
from jax import lax

D = 2048
HEADS = 8
HD = 128
FF = 1408
TOP = 2
POS = 256
EXPERTS = 128
CLIPS = 8
FRAMES = 16
HH = 1024
CAP = 8


def draw_tokens(key, part):
    full_shape = (CLIPS, FRAMES, POS, D)
    values = jnp.clip(jax.random.normal(jax.random.fold_in(key, 11), full_shape, jnp.float32), -6.0, 6.0)
    return values.astype(jnp.bfloat16)


def spatial_pair(key):
    base_key = jax.random.fold_in(key, 3131)
    full_shape = (CLIPS, FRAMES, POS, HEADS, HD)
    query_side = jnp.clip(jax.random.normal(jax.random.fold_in(base_key, 1), full_shape, jnp.float32), -4.5, 4.5)
    key_side = jnp.clip(jax.random.normal(jax.random.fold_in(base_key, 2), full_shape, jnp.float32), -4.5, 4.5)
    flat_shape = (CLIPS, FRAMES, POS, HEADS * HD)
    return (query_side.reshape(flat_shape), key_side.reshape(flat_shape))


def draw_spatial_queries(key, part):
    query_side, key_side = spatial_pair(key)
    return query_side.astype(jnp.bfloat16)


def draw_spatial_keys(key, part):
    query_side, key_side = spatial_pair(key)
    return key_side.astype(jnp.bfloat16)


def draw_temporal_qkv(key, part):
    fan_scale = 1.0 / math.sqrt(D)
    full_shape = (D, 3, HEADS, HD)
    values = jax.random.normal(jax.random.fold_in(key, 21), full_shape, jnp.float32) * fan_scale
    values = jnp.clip(values, -6.0 * fan_scale, 6.0 * fan_scale)
    return values.reshape(D, 3 * HEADS * HD).astype(jnp.bfloat16)


def draw_frame_mask(key, part):
    coin_flips = jax.random.randint(jax.random.fold_in(key, 55), (CLIPS, FRAMES, FRAMES), 0, 2)
    row_index = jnp.arange(FRAMES, dtype=jnp.int32)[:, None]
    col_index = jnp.arange(FRAMES, dtype=jnp.int32)[None, :]
    diagonal = jnp.where(col_index == row_index, 1, 0)
    return jnp.where(col_index < row_index, coin_flips, diagonal[None, :, :]).astype(jnp.int32)


def block_levels(own_key, shape, cuts, low, high):
    loudness = 1.0
    for dim, shards_of in cuts:
        draws = jax.random.uniform(jax.random.fold_in(jax.random.fold_in(own_key, 6), dim), (shards_of,), jnp.float32, low / len(cuts), high / len(cuts))
        loudness = loudness * jnp.repeat(jnp.exp(draws), shape[dim] // shards_of).reshape((-1,) + (1,) * (len(shape) - 1 - dim))
    return loudness


def deal_out(key, own, number, rows, number_of, top, reach, lean):
    order = jax.random.permutation(key, number_of)
    heavy_load, common = load_shares(number_of, rows * top, reach, lean, True), load_shares(number_of, rows * top, reach, lean, False)
    places = jnp.arange(number_of)

    def named(tallies, rotation):
        used = int((tallies > 0).sum())
        fixed = max(1, used // 4)
        passed = fixed + (places - fixed + rotation * (used - fixed)) % max(1, number_of - fixed)
        return jnp.zeros((number_of,), jnp.int32).at[order[jnp.where(places < fixed, places, passed)]].set(jnp.asarray(tallies, jnp.int32))

    tallies = jnp.where(number % 4 == 0, named(heavy_load, number // 4), named(common, number - number // 4 - 1))
    mixed = jax.random.permutation(jax.random.fold_in(own, 3), number_of)
    donor, taker = mixed[0:number_of // 2 * 2:2], mixed[1:number_of // 2 * 2:2]
    slack = jnp.minimum(tallies[donor] - 1, reach - tallies[taker]) // 2
    slack = jnp.where((donor == order[0]) | (taker == order[0]) | (tallies[taker] == 0), 0, jnp.maximum(slack, 0))
    passed = jax.random.randint(jax.random.fold_in(own, 4), (number_of // 2,), 0, 1 << 20) % (slack + 1)
    tallies = tallies.at[donor].add(-passed).at[taker].add(passed)
    labels = jnp.searchsorted(jnp.cumsum(tallies), jnp.arange(rows * top), side="right").astype(jnp.int32)
    table = labels.reshape(top, rows).T
    table = table[jax.random.permutation(jax.random.fold_in(own, 1), rows)]
    rotation = jax.random.randint(jax.random.fold_in(own, 2), (rows, 1), 0, top)
    return jnp.take_along_axis(table, (jnp.arange(top)[None, :] + rotation) % top, axis=1)


def load_shares(amount, total, bound, skew, full):
    loads = [(1 << 20) // math.isqrt(grade ** skew) + 1 for grade in range(1, amount + 1)]
    largest = bound if full else min(bound, max(-(-total // amount), total * loads[0] // sum(loads)))
    least = 1 if total - largest >= amount - 1 else 0
    given, spare = [largest] + [least] * (amount - 1), total - largest - least * (amount - 1)
    while spare > 0:
        movable = [i for i in range(1, amount) if given[i] < largest] or [i for i in range(1, amount) if given[i] < bound]
        whole, left = sum([loads[i] for i in movable]), spare
        for i in movable:
            more = min(bound - given[i], max(1, left * loads[i] // whole), spare)
            given[i] = given[i] + more
            spare = spare - more
    return np.array(given)


def gaussian(key, shape, deviation, reach, cuts=(), kind=jnp.bfloat16):
    entries = jax.random.normal(key, shape, jnp.float32) * deviation
    if len(cuts) > 0:
        entries = block_levels(key, shape, cuts, -0.22, 0.18) * entries
    return jnp.clip(entries, min=-reach, max=reach).astype(kind)


def setup_inputs(seed: int = 0) -> dict:
    key_list = jax.random.split(jax.random.key(seed), 14)
    tokens = draw_tokens(jax.random.fold_in(key_list[13], 71), 0)
    spatial_queries = draw_spatial_queries(jax.random.fold_in(key_list[13], 71), 0)
    spatial_keys = draw_spatial_keys(jax.random.fold_in(key_list[13], 71), 0)
    spatial_values = gaussian(key_list[3], (CLIPS, FRAMES, POS, HH), 1.0, 6.0, ((0, 8), (1, 16)))
    spatial_proj = gaussian(key_list[4], (HH, D), HH ** -0.5, 0.1875, ((0, 16),))
    temporal_qkv = draw_temporal_qkv(jax.random.fold_in(key_list[13], 71), 0)
    temporal_proj = gaussian(key_list[6], (HH, D), HH ** -0.5, 0.1875, ((0, 16),))
    frame_mask = draw_frame_mask(jax.random.fold_in(key_list[13], 71), 0)
    expert_ids_keys = jax.random.split(jax.random.fold_in(key_list[8], 1), CLIPS * FRAMES * POS // POS)
    expert_ids_turns = jax.random.permutation(jax.random.fold_in(key_list[8], 3), CLIPS * FRAMES * POS // POS)
    expert_ids = jax.vmap(lambda own, number: deal_out(jax.random.fold_in(key_list[8], 2), own, number, POS, EXPERTS, TOP, CAP, 2))(expert_ids_keys, expert_ids_turns).reshape((CLIPS, FRAMES, POS, TOP))
    gate_values = jnp.clip(0.2 + 0.8 * jax.random.uniform(key_list[9], (CLIPS, FRAMES, POS, TOP), jnp.float32) ** block_levels(key_list[9], (CLIPS, FRAMES, POS, TOP), ((0, 8), (1, 16)), -0.2, 0.2), 0.2, 1.0)
    expert_gate = gaussian(key_list[10], (EXPERTS, D, FF), D ** -0.5, 0.125, ((0, 128),))
    expert_up = gaussian(key_list[11], (EXPERTS, D, FF), D ** -0.5, 0.125, ((0, 128),))
    expert_down = gaussian(key_list[12], (EXPERTS, FF, D), FF ** -0.5, 0.15625, ((0, 128),))
    return {"tokens": tokens, "spatial_queries": spatial_queries, "spatial_keys": spatial_keys, "spatial_values": spatial_values, "spatial_proj": spatial_proj, "temporal_qkv": temporal_qkv, "temporal_proj": temporal_proj, "frame_mask": frame_mask, "expert_ids": expert_ids, "gate_values": gate_values, "expert_gate": expert_gate, "expert_up": expert_up, "expert_down": expert_down}


EPS = 1e-06
MASKED = -1e+30

def rms_normed(values):
    wide = values.astype(jnp.float32)
    inverse = lax.rsqrt(lax.optimization_barrier(jnp.mean(wide * wide, axis=-1, keepdims=True)) + EPS)
    return (wide * inverse).astype(jnp.bfloat16)

def normalize_rows(scores):
    row_max = lax.optimization_barrier(jnp.max(scores, axis=-1, keepdims=True))
    exp_terms = jnp.exp(scores - row_max)
    return (exp_terms / lax.optimization_barrier(jnp.sum(exp_terms, axis=-1, keepdims=True))).astype(jnp.bfloat16)

def spatial_clip(triple):
    queries, keys, values = triple
    score_scale = 1.0 / math.sqrt(HD)
    query_heads = queries.astype(jnp.float32).reshape(FRAMES, POS, HEADS, HD)
    key_heads = keys.astype(jnp.float32).reshape(FRAMES, POS, HEADS, HD)
    value_heads = values.astype(jnp.float32).reshape(FRAMES, POS, HEADS, HD)
    scores = jnp.einsum('fqhd,fkhd->fhqk', query_heads, key_heads) * score_scale
    weights = normalize_rows(scores)
    mixed = jnp.einsum('fhqk,fkhd->fqhd', weights.astype(jnp.float32), value_heads)
    return mixed.astype(jnp.bfloat16).reshape(FRAMES, POS, HEADS * HD)

def reference(tokens, spatial_queries, spatial_keys, spatial_values, spatial_proj, temporal_qkv, temporal_proj, frame_mask, expert_ids, gate_values, expert_gate, expert_up, expert_down):
    score_scale = 1.0 / math.sqrt(HD)
    spatial_mixed = lax.map(spatial_clip, (spatial_queries, spatial_keys, spatial_values))
    spatial_update = jnp.dot(spatial_mixed.reshape(-1, HEADS * HD), spatial_proj, preferred_element_type=jnp.float32)
    first = (tokens.reshape(-1, D).astype(jnp.float32) + spatial_update).astype(jnp.bfloat16)
    normed = rms_normed(first)
    triple = jnp.dot(normed, temporal_qkv, preferred_element_type=jnp.float32).astype(jnp.bfloat16)
    triple = triple.reshape(CLIPS, FRAMES, POS, 3, HEADS, HD).astype(jnp.float32)
    scores = jnp.einsum('ciphd,cjphd->cphij', triple[:, :, :, 0], triple[:, :, :, 1]) * score_scale
    allowed = (frame_mask == 1)[:, None, None, :, :]
    weights = normalize_rows(jnp.where(allowed, scores, MASKED))
    temporal_mixed = jnp.einsum('cphij,cjphd->ciphd', weights.astype(jnp.float32), triple[:, :, :, 2])
    temporal_mixed = temporal_mixed.astype(jnp.bfloat16).reshape(-1, HEADS * HD)
    temporal_update = jnp.dot(temporal_mixed, temporal_proj, preferred_element_type=jnp.float32).astype(jnp.bfloat16)
    second = (first.astype(jnp.float32) + temporal_update.astype(jnp.float32)).astype(jnp.bfloat16)
    routed = rms_normed(second)
    pair_ids = expert_ids.reshape(-1).astype(jnp.int32)
    pair_total = pair_ids.shape[0]
    ordering = jnp.argsort(pair_ids, stable=True).astype(jnp.int32)
    sorted_ids = pair_ids[ordering]
    counts = lax.optimization_barrier(jnp.sum((pair_ids[:, None] == jnp.arange(EXPERTS, dtype=jnp.int32)[None, :]).astype(jnp.int32), axis=0))
    starts = (jnp.cumsum(counts) - counts).astype(jnp.int32)
    rank_sorted = (jnp.arange(pair_total, dtype=jnp.int32) - starts[sorted_ids]).astype(jnp.int32)
    slot_table = jnp.full((EXPERTS, EXPERTS * CAP), -1, jnp.int32).at[sorted_ids, rank_sorted].set(ordering)
    rank_pair = jnp.zeros((pair_total,), jnp.int32).at[ordering].set(rank_sorted)

    def one_expert(pieces):
        pair_index, gate_rows, up_rows, down_rows = pieces
        present = pair_index >= 0
        token_index = (jnp.maximum(pair_index, 0) // TOP).astype(jnp.int32)
        token_rows = jnp.where(present[:, None], routed[token_index], jnp.zeros((), jnp.bfloat16))
        gate_part = jnp.dot(token_rows, gate_rows, preferred_element_type=jnp.float32)
        up_part = jnp.dot(token_rows, up_rows, preferred_element_type=jnp.float32)
        hidden = (jax.nn.silu(gate_part) * up_part).astype(jnp.bfloat16)
        return jnp.dot(hidden, down_rows, preferred_element_type=jnp.float32).astype(jnp.bfloat16)
    answers = lax.map(one_expert, (slot_table, expert_gate, expert_up, expert_down))
    pair_answers = answers[pair_ids, rank_pair].astype(jnp.float32).reshape(-1, TOP, D)
    expert_mix = lax.optimization_barrier(jnp.sum(pair_answers * gate_values.reshape(-1, TOP, 1), axis=1))
    layer_out = (second.astype(jnp.float32) + expert_mix).astype(jnp.bfloat16)
    return layer_out.reshape(CLIPS, FRAMES, POS, D)
```

```python
import functools
import math

import jax
import jax.numpy as jnp
from jax import lax
from jax.experimental import pallas as pl
from jax.experimental.pallas import tpu as pltpu
from jax.sharding import PartitionSpec as P

HEADS = 8
HD = 128
TOP = 2
SIDE = 4
TM = 16


EPS = 1e-06
MASKED = -1e30
MESH = pl.DeviceIdType.MESH


def grouped_exchange(x, axis, split_dim, concat_dim, work, item_dim, out_dim):

    def moved(group):
        return lax.all_to_all(group, axis, split_axis=split_dim, concat_axis=concat_dim, tiled=True)

    items = jax.tree.leaves(x)[0].shape[item_dim]
    ends = [items * k // 2 for k in range(2 + 1)] if items % 2 == 0 else [0, items]
    groups = [
        jax.tree.map(lambda a: lax.slice_in_dim(a, low, high, axis=item_dim), x)
        for low, high in zip(ends, ends[1:])
    ]
    arrived = [moved(group) for group in groups]
    made = [work(group) for group in arrived]
    return jax.tree.map(lambda *parts: jnp.concatenate(parts, axis=out_dim), *made)


class Gather:
    def __init__(self, shard, full, place, send, recv):
        self.shard, self.full, self.send, self.recv = shard, full, send, recv
        self.rows = full.shape[1]
        self.place = place

    def part(self, index, quarter=None):
        half = self.rows // 2
        if quarter is None:
            start = pl.multiple_of(self.place["core"] * half, half)
            return self.full.at[index, pl.ds(start, half)]
        size = half // 2
        start = pl.multiple_of(self.place["core"] * half + quarter * size, size)
        return self.full.at[index, pl.ds(start, size)]

    def own_part(self):
        half = self.rows // 2
        start = pl.multiple_of(self.place["core"] * half, half)
        return self.shard.at[pl.ds(start, half)]

    def at(self, step1, step2):
        p = self.place
        return lax.rem(p["i1"] + step1 + SIDE, SIDE) * p["s1"] + lax.rem(p["i2"] + step2 + SIDE, SIDE) * p["s2"]

    def copy(self, src, dst, slot, clip, tm):
        pltpu.make_async_remote_copy(
            src_ref=src,
            dst_ref=dst,
            send_sem=self.send,
            recv_sem=self.recv.at[slot],
            device_id=(clip, tm),
            device_id_type=MESH,
        ).start()

    def arrived(self, ref, slot):
        pltpu.make_async_copy(ref, ref, self.recv.at[slot]).wait()

    def along(self, dim, way, src, dst, slot):
        target = self.at(way, 0) if dim == 1 else self.at(0, way)
        self.copy(src, dst, slot, self.place["clip"], target)

    def push(self, src, dst):
        self.copy(src, dst, 20, self.place["partner"], self.place["tm"])

    OFFSETS = (0, -1, 1, 2)

    def second_dim(self, k):
        index = self.at(self.OFFSETS[k], 0)
        src = self.own_part() if k == 0 else self.part(index)
        self.along(2, 1, src, self.part(index), 4 + 2 * k)
        self.along(2, -1, src, self.part(index), 5 + 2 * k)
        if k > 0:
            self.push(self.part(index), self.part(index))

    def own(self):
        mine = self.part(self.place["tm"])
        self.along(1, 1, self.own_part(), mine, 0)
        self.along(1, -1, self.own_part(), mine, 1)
        self.second_dim(0)

    def first_near(self):
        low, high = self.at(-1, 0), self.at(1, 0)
        self.arrived(self.part(low), 0)
        self.along(1, 1, self.part(low, 0), self.part(low, 0), 2)
        self.second_dim(1)
        self.arrived(self.part(high), 1)
        self.along(1, -1, self.part(high, 1), self.part(high, 1), 3)
        self.second_dim(2)

    def first_far(self):
        far = self.at(2, 0)
        self.arrived(self.part(far, 0), 2)
        self.arrived(self.part(far, 1), 3)
        self.second_dim(3)

    def second_near(self, k):
        step = self.OFFSETS[k]
        low, high = self.at(step, -1), self.at(step, 1)
        self.arrived(self.part(low), 4 + 2 * k)
        self.along(2, 1, self.part(low, 0), self.part(low, 0), 12 + 2 * k)
        self.push(self.part(low), self.part(low))
        self.arrived(self.part(high), 5 + 2 * k)
        self.along(2, -1, self.part(high, 1), self.part(high, 1), 13 + 2 * k)
        self.push(self.part(high), self.part(high))

    def second_far(self, k):
        far = self.at(self.OFFSETS[k], 2)
        self.arrived(self.part(far, 0), 12 + 2 * k)
        self.arrived(self.part(far, 1), 13 + 2 * k)
        self.push(self.part(far), self.part(far))

    def pushed(self):
        half = self.rows // 2
        ref = self.full.at[pl.ds(0, TM - 1), pl.ds(0, half)]
        self.arrived(ref, 20)

    def drained(self):
        ref = self.full.at[pl.ds(0, TM - 1)]
        pltpu.make_async_copy(ref, ref, self.send).wait()


def normed_rows(ref, out):
    def step(block, carry):
        rows = pl.ds(pl.multiple_of(block * 32, 32), 32)
        wide = ref[rows, :].astype(jnp.float32)
        inverse = lax.rsqrt(jnp.mean(wide * wide, axis=-1, keepdims=True) + EPS)
        out[rows, :] = (wide * inverse).astype(jnp.bfloat16)
        return carry

    lax.fori_loop(0, ref.shape[0] // 32, step, 0)


def attend(queries, keys, values, out, bias, heads):
    scale = 1.0 / math.sqrt(HD)

    def step(index, carry):
        for head in (2 * index, 2 * index + 1):
            cols = pl.ds(pl.multiple_of(head * HD, HD), HD)
            scores = lax.dot_general(
                queries[:, cols], keys[:, cols], (((1,), (1,)), ((), ())), preferred_element_type=jnp.float32
            )
            scores = scores * scale
            if bias is not None:
                scores = jnp.where(bias[...] > 0.5, scores, MASKED)
            top = jnp.max(scores, axis=-1, keepdims=True)
            terms = jnp.exp(scores - top)
            weights = (terms * (1.0 / jnp.sum(terms, axis=-1, keepdims=True))).astype(jnp.bfloat16)
            mixed = jnp.dot(weights, values[:, cols], preferred_element_type=jnp.float32)
            out[:, cols] = mixed.astype(jnp.bfloat16)
        return carry

    lax.fori_loop(0, heads // 2, step, 0)


def trunk_kernel(
    tokens, sq, sk, sv, sproj, tqkv, tproj, mask,
    second_out, routed_out,
    tok_v, q_v, k_v, v_v, mixed_v, first_v, normed_v, spread_v, qkv_v, home_v, allowed_v, mask_v,
    wide_v, proj_s, qkv_w, proj_t,
    local_sem, send_sem, recv_s, recv_q, recv_t, swap_send, swap_recv, out_sem,
):
    clip = lax.axis_index("clip")
    tm = lax.axis_index("tm")
    core = lax.rem(clip, 2)
    y, x = tm // SIDE, lax.rem(tm, SIDE)
    positions = tok_v.shape[0]
    per = positions // TM
    place = {
        "clip": clip,
        "tm": tm,
        "core": core,
        "partner": clip + 1 - 2 * core,
        "i1": x * (1 - core) + y * core,
        "i2": y * (1 - core) + x * core,
        "s1": 1 + 3 * core,
        "s2": 4 - 3 * core,
    }
    spatial = Gather(sproj, proj_s, place, send_sem.at[0], recv_s)
    qkv = Gather(tqkv, qkv_w, place, send_sem.at[1], recv_q)
    temporal = Gather(tproj, proj_t, place, send_sem.at[2], recv_t)

    loads = [
        pltpu.make_async_copy(src, dst, local_sem.at[n])
        for n, (src, dst) in enumerate(
            [
                (sq, q_v), (sk, k_v), (sv, v_v), (tokens, tok_v),
                (sproj, proj_s.at[tm]), (tqkv, qkv_w.at[tm]), (tproj, proj_t.at[tm]), (mask, mask_v),
            ]
        )
    ]
    for load in loads:
        load.start()

    barrier = pltpu.get_barrier_semaphore()

    def greet(step, carry):
        pl.semaphore_signal(
            barrier, inc=1, device_id=(clip, lax.rem(tm + step, TM)), device_id_type=MESH
        )
        return carry

    lax.fori_loop(1, TM, greet, 0)
    pl.semaphore_signal(barrier, inc=1, device_id=(place["partner"], tm), device_id_type=MESH)
    pl.semaphore_wait(barrier, TM)

    spatial.own()
    qkv.own()

    for n in (0, 1, 2):
        loads[n].wait()
    attend(q_v, k_v, v_v, mixed_v, None, HEADS)

    spatial.first_near()
    spatial.first_far()
    qkv.first_near()
    temporal.own()
    for k in range(4):
        spatial.second_near(k)
    for k in range(4):
        spatial.second_far(k)
    qkv.first_far()
    loads[3].wait()
    loads[4].wait()
    spatial.pushed()

    model = tok_v.shape[1]
    width = 512

    def project(chunk, carry):
        cols = pl.ds(pl.multiple_of(chunk * width, width), width)
        weights = proj_s[:, :, cols].reshape(mixed_v.shape[1], width)
        update = jnp.dot(mixed_v[...], weights, preferred_element_type=jnp.float32)
        first_v[:, cols] = (tok_v[:, cols].astype(jnp.float32) + update).astype(jnp.bfloat16)
        return carry

    lax.fori_loop(0, model // width, project, 0)
    normed_rows(first_v, normed_v)

    def swap(src_of, dst, slot):
        def step(shift, carry):
            other = lax.rem(tm + shift, TM)
            pltpu.make_async_remote_copy(
                src_ref=src_of(other),
                dst_ref=dst.at[tm],
                send_sem=swap_send.at[slot],
                recv_sem=swap_recv.at[slot],
                device_id=(clip, other),
                device_id_type=MESH,
            ).start()
            return carry

        lax.fori_loop(1, TM, step, 0)
        kept = pltpu.make_async_copy(src_of(tm), dst.at[tm], local_sem.at[8 + slot])
        kept.start()
        return kept

    def swapped(dst, kept, slot):
        ref = dst.at[pl.ds(0, TM - 1)]
        pltpu.make_async_copy(ref, ref, swap_recv.at[slot]).wait()
        kept.wait()

    def block_of(ref):
        return lambda index: ref.at[pl.ds(pl.multiple_of(index * per, per), per)]

    kept = swap(block_of(normed_v), spread_v, 0)

    temporal.first_near()
    for k in range(4):
        qkv.second_near(k)
    temporal.first_far()
    for k in range(4):
        qkv.second_far(k)

    rows = lax.broadcasted_iota(jnp.int32, (positions, TM), 0) // per
    cols16 = lax.broadcasted_iota(jnp.int32, (positions, TM), 1)
    frame_of = (rows == cols16).astype(jnp.float32)
    loads[7].wait()
    mask_f = jnp.where(mask_v[...] == 1, 1.0, 0.0)
    by_row = jnp.dot(frame_of, mask_f, preferred_element_type=jnp.float32)
    pairs = lax.dot_general(by_row, frame_of, (((1,), (1,)), ((), ())), preferred_element_type=jnp.float32)
    pos_r = lax.rem(lax.broadcasted_iota(jnp.int32, (positions, positions), 0), per)
    pos_c = lax.rem(lax.broadcasted_iota(jnp.int32, (positions, positions), 1), per)
    allowed_v[...] = jnp.where(pos_r == pos_c, pairs, 0.0)

    loads[5].wait()
    qkv.pushed()
    swapped(spread_v, kept, 0)

    def triple(chunk):
        cols = pl.ds(chunk * width, width)
        weights = qkv_w[:, :, cols].reshape(model, width)
        rows_in = spread_v[...].reshape(positions, model)
        qkv_v[:, cols] = jnp.dot(rows_in, weights, preferred_element_type=jnp.float32).astype(jnp.bfloat16)

    head_width = HEADS * HD
    for chunk in range(3 * head_width // width):
        triple(chunk)
        if chunk < 4:
            temporal.second_near(chunk)

    attend(
        qkv_v.at[:, pl.ds(0, head_width)],
        qkv_v.at[:, pl.ds(head_width, head_width)],
        qkv_v.at[:, pl.ds(2 * head_width, head_width)],
        wide_v, allowed_v, HEADS,
    )
    kept = swap(block_of(wide_v), home_v, 1)
    for k in range(4):
        temporal.second_far(k)
    loads[6].wait()
    temporal.pushed()
    swapped(home_v, kept, 1)

    def finish(chunk, carry):
        cols = pl.ds(pl.multiple_of(chunk * width, width), width)
        weights = proj_t[:, :, cols].reshape(head_width, width)
        rows_in = home_v[...].reshape(positions, head_width)
        update = jnp.dot(rows_in, weights, preferred_element_type=jnp.float32).astype(jnp.bfloat16)
        tok_v[:, cols] = (
            first_v[:, cols].astype(jnp.float32) + update.astype(jnp.float32)
        ).astype(jnp.bfloat16)
        return carry

    lax.fori_loop(0, model // width, finish, 0)
    put = pltpu.make_async_copy(tok_v, second_out, out_sem.at[0])
    put.start()
    ref = normed_v.at[pl.ds(0, positions - per)]
    pltpu.make_async_copy(ref, ref, swap_send.at[0]).wait()
    normed_rows(tok_v, normed_v)
    put2 = pltpu.make_async_copy(normed_v, routed_out, out_sem.at[1])
    put2.start()
    ref = wide_v.at[pl.ds(0, positions - per)]
    pltpu.make_async_copy(ref, ref, swap_send.at[1]).wait()
    spatial.drained()
    qkv.drained()
    temporal.drained()
    put.wait()
    put2.wait()


def trunk(tokens, sq, sk, sv, sproj, tqkv, tproj, mask):
    positions, model = tokens.shape
    head_width = sq.shape[1]
    per = positions // TM
    bf16 = jnp.bfloat16
    vm = lambda *shape: pltpu.VMEM(shape, bf16)
    any_spec = pl.BlockSpec(memory_space=pl.ANY)
    return pl.pallas_call(
        trunk_kernel,
        out_shape=(jax.ShapeDtypeStruct((positions, model), bf16),) * 2,
        in_specs=[any_spec] * 8,
        out_specs=(any_spec,) * 2,
        scratch_shapes=[
            vm(positions, model), vm(positions, head_width), vm(positions, head_width), vm(positions, head_width),
            vm(positions, head_width), vm(positions, model), vm(positions, model), vm(TM, per, model),
            vm(positions, 3 * head_width), vm(TM, per, head_width),
            pltpu.VMEM((positions, positions), jnp.float32), pltpu.VMEM((TM, TM), jnp.int32),
            vm(positions, head_width),
            vm(TM, sproj.shape[0], model), vm(TM, tqkv.shape[0], 3 * head_width), vm(TM, tproj.shape[0], model),
            pltpu.SemaphoreType.DMA((10,)), pltpu.SemaphoreType.DMA((3,)),
            pltpu.SemaphoreType.DMA((21,)), pltpu.SemaphoreType.DMA((21,)), pltpu.SemaphoreType.DMA((21,)),
            pltpu.SemaphoreType.DMA((2,)), pltpu.SemaphoreType.DMA((2,)), pltpu.SemaphoreType.DMA((2,)),
        ],
        compiler_params=pltpu.CompilerParams(
            collective_id=0, has_side_effects=True, vmem_limit_bytes=60 * 1024 * 1024
        ),
        name="trunk",
    )(tokens, sq, sk, sv, sproj, tqkv, tproj, mask)


def shards(
    tokens,
    spatial_queries,
    spatial_keys,
    spatial_values,
    spatial_proj,
    temporal_qkv,
    temporal_proj,
    frame_mask,
    expert_ids,
    gate_values,
    expert_gate,
    expert_up,
    expert_down,
):
    model_width = tokens.shape[3]
    positions = tokens.shape[2]
    tm_count = lax.axis_size("tm")
    clip_count = lax.axis_size("clip")
    experts = clip_count * tm_count
    second, routed = trunk(
        tokens.reshape(positions, model_width),
        spatial_queries.reshape(positions, -1),
        spatial_keys.reshape(positions, -1),
        spatial_values.reshape(positions, -1),
        spatial_proj,
        temporal_qkv,
        temporal_proj,
        frame_mask.reshape(frame_mask.shape[1:]),
    )
    capacity = 2 * TOP * positions // experts
    slot_count = experts * capacity
    pair_ids = expert_ids.reshape(positions * TOP)
    chosen = (pair_ids[:, None] == jnp.arange(experts, dtype=jnp.int32)[None, :]).astype(jnp.int32)
    earlier = jnp.cumsum(chosen, axis=0) - chosen
    pair_rank = jnp.sum(earlier * chosen, axis=1)
    pair_slot = pair_ids * capacity + pair_rank
    slot_index = jnp.arange(slot_count, dtype=jnp.int32)
    pair_onehot = (pair_slot[:, None] == slot_index[None, :]).astype(jnp.bfloat16)
    token_onehot = jnp.any(
        pair_slot.reshape(positions, TOP)[:, :, None] == slot_index[None, None, :], axis=1
    ).astype(jnp.bfloat16)
    outgoing = lax.dot_general(
        token_onehot, routed, (((0,), (0,)), ((), ())), preferred_element_type=jnp.float32
    )
    outgoing = outgoing.astype(jnp.bfloat16).reshape(experts, capacity, model_width)

    def expert_rows(received):
        flat_rows = received.reshape(-1, model_width)
        gate_part = jnp.dot(flat_rows, expert_gate[0], preferred_element_type=jnp.float32)
        up_part = jnp.dot(flat_rows, expert_up[0], preferred_element_type=jnp.float32)
        hidden = (jax.nn.silu(gate_part) * up_part).astype(jnp.bfloat16)
        answer = jnp.dot(hidden, expert_down[0], preferred_element_type=jnp.float32).astype(
            jnp.bfloat16
        )
        return answer.reshape(received.shape)

    def serve_slots(received):
        return lax.all_to_all(
            expert_rows(received), ("clip", "tm"), split_axis=0, concat_axis=0, tiled=True
        )

    answers = grouped_exchange(outgoing, ("clip", "tm"), 0, 0, serve_slots, 1, 1)
    pair_answers = jnp.dot(
        pair_onehot, answers.reshape(slot_count, model_width), preferred_element_type=jnp.float32
    )
    weighted = pair_answers.reshape(positions, TOP, model_width) * gate_values.reshape(
        positions, TOP, 1
    )
    expert_mix = jnp.sum(weighted, axis=1)
    layer_out = (second.astype(jnp.float32) + expert_mix).astype(jnp.bfloat16)
    return layer_out.reshape(tokens.shape)


def solution(mesh):
    placed = (
        P("clip", "tm", None, None),
        P("clip", "tm", None, None),
        P("clip", "tm", None, None),
        P("clip", "tm", None, None),
        P("tm", None),
        P("tm", None),
        P("tm", None),
        P("clip", None, None),
        P("clip", "tm", None, None),
        P("clip", "tm", None, None),
        P(("clip", "tm"), None, None),
        P(("clip", "tm"), None, None),
        P(("clip", "tm"), None, None),
    )
    return jax.shard_map(
        shards, mesh=mesh, in_specs=placed, out_specs=P("clip", "tm", None, None), check_vma=False
    )
```

```python
import math

import jax
import jax.numpy as jnp
from jax import lax
from jax.experimental import pallas as pl
from jax.experimental.pallas import tpu as pltpu
from jax.sharding import PartitionSpec as P

HEADS = 8
HD = 128
TOP = 2
CAP = 8
SIDE = 4
TM = 16


EPS = 1e-06
MASKED = -1e30
MESH = pl.DeviceIdType.MESH
STRIDE = 49
INVERSE = pow(STRIDE, -1, 128)
GROUPS = 4
DEVICES = 128


class Gather:
    def __init__(self, shard, full, place, send, recv):
        self.shard, self.full, self.send, self.recv = shard, full, send, recv
        self.rows = full.shape[1]
        self.place = place

    def part(self, index, quarter=None):
        half = self.rows // 2
        if quarter is None:
            start = pl.multiple_of(self.place["core"] * half, half)
            return self.full.at[index, pl.ds(start, half)]
        size = half // 2
        start = pl.multiple_of(self.place["core"] * half + quarter * size, size)
        return self.full.at[index, pl.ds(start, size)]

    def own_part(self):
        half = self.rows // 2
        start = pl.multiple_of(self.place["core"] * half, half)
        return self.shard.at[pl.ds(start, half)]

    def at(self, step1, step2):
        p = self.place
        return lax.rem(p["i1"] + step1 + SIDE, SIDE) * p["s1"] + lax.rem(p["i2"] + step2 + SIDE, SIDE) * p["s2"]

    def copy(self, src, dst, slot, clip, tm):
        pltpu.make_async_remote_copy(
            src_ref=src,
            dst_ref=dst,
            send_sem=self.send,
            recv_sem=self.recv.at[slot],
            device_id=(clip, tm),
            device_id_type=MESH,
        ).start()

    def arrived(self, ref, slot):
        pltpu.make_async_copy(ref, ref, self.recv.at[slot]).wait()

    def along(self, dim, way, src, dst, slot):
        target = self.at(way, 0) if dim == 1 else self.at(0, way)
        self.copy(src, dst, slot, self.place["clip"], target)

    def push(self, src, dst):
        self.copy(src, dst, 20, self.place["partner"], self.place["tm"])

    OFFSETS = (0, -1, 1, 2)

    def second_dim(self, k):
        index = self.at(self.OFFSETS[k], 0)
        src = self.own_part() if k == 0 else self.part(index)
        self.along(2, 1, src, self.part(index), 4 + 2 * k)
        self.along(2, -1, src, self.part(index), 5 + 2 * k)
        if k > 0:
            self.push(self.part(index), self.part(index))

    def own(self):
        mine = self.part(self.place["tm"])
        self.along(1, 1, self.own_part(), mine, 0)
        self.along(1, -1, self.own_part(), mine, 1)
        self.second_dim(0)

    def first_near(self):
        low, high = self.at(-1, 0), self.at(1, 0)
        self.arrived(self.part(low), 0)
        self.along(1, 1, self.part(low, 0), self.part(low, 0), 2)
        self.second_dim(1)
        self.arrived(self.part(high), 1)
        self.along(1, -1, self.part(high, 1), self.part(high, 1), 3)
        self.second_dim(2)

    def first_far(self):
        far = self.at(2, 0)
        self.arrived(self.part(far, 0), 2)
        self.arrived(self.part(far, 1), 3)
        self.second_dim(3)

    def second_near(self, k):
        step = self.OFFSETS[k]
        low, high = self.at(step, -1), self.at(step, 1)
        self.arrived(self.part(low), 4 + 2 * k)
        self.along(2, 1, self.part(low, 0), self.part(low, 0), 12 + 2 * k)
        self.push(self.part(low), self.part(low))
        self.arrived(self.part(high), 5 + 2 * k)
        self.along(2, -1, self.part(high, 1), self.part(high, 1), 13 + 2 * k)
        self.push(self.part(high), self.part(high))

    def second_far(self, k):
        far = self.at(self.OFFSETS[k], 2)
        self.arrived(self.part(far, 0), 12 + 2 * k)
        self.arrived(self.part(far, 1), 13 + 2 * k)
        self.push(self.part(far), self.part(far))

    def pushed(self):
        half = self.rows // 2
        ref = self.full.at[pl.ds(0, TM - 1), pl.ds(0, half)]
        self.arrived(ref, 20)

    def drained(self):
        ref = self.full.at[pl.ds(0, TM - 1)]
        pltpu.make_async_copy(ref, ref, self.send).wait()


def normed_rows(ref, out):
    def step(block, carry):
        rows = pl.ds(pl.multiple_of(block * 32, 32), 32)
        wide = ref[rows, :].astype(jnp.float32)
        inverse = lax.rsqrt(jnp.mean(wide * wide, axis=-1, keepdims=True) + EPS)
        out[rows, :] = (wide * inverse).astype(jnp.bfloat16)
        return carry

    lax.fori_loop(0, ref.shape[0] // 32, step, 0)


def attend(queries, keys, values, out, bias, heads):
    scale = 1.0 / math.sqrt(HD)

    def step(index, carry):
        for head in (2 * index, 2 * index + 1):
            cols = pl.ds(pl.multiple_of(head * HD, HD), HD)
            scores = lax.dot_general(
                queries[:, cols], keys[:, cols], (((1,), (1,)), ((), ())), preferred_element_type=jnp.float32
            )
            scores = scores * scale
            if bias is not None:
                scores = jnp.where(bias[...] > 0.5, scores, MASKED)
            top = jnp.max(scores, axis=-1, keepdims=True)
            terms = jnp.exp(scores - top)
            weights = (terms * (1.0 / jnp.sum(terms, axis=-1, keepdims=True))).astype(jnp.bfloat16)
            mixed = jnp.dot(weights, values[:, cols], preferred_element_type=jnp.float32)
            out[:, cols] = mixed.astype(jnp.bfloat16)
        return carry

    lax.fori_loop(0, heads // 2, step, 0)


def layer_kernel(
    tokens, sq, sk, sv, sproj, tqkv, tproj, mask, ids, gates, w_gate, w_up, w_down,
    out,
    tok_v, mixed_v, normed_v, spread_v, qkv_v, home_v, allowed_v, mask_v, ids_v, gates_v,
    proj_s, qkv_w, proj_t, gate_w, up_w, down_w, outgoing, received, answers, hidden_v, total_v,
    slots_v, slots_t,
    local_sem, send_sem, recv_s, recv_q, recv_t, swap_send, swap_recv, moe_send, go_recv, back_recv,
):
    clip = lax.axis_index("clip")
    tm = lax.axis_index("tm")
    core = lax.rem(clip, 2)
    y, x = tm // SIDE, lax.rem(tm, SIDE)
    positions = tok_v.shape[0]
    per = positions // TM
    head_width = HEADS * HD
    me = clip * TM + tm
    place = {
        "clip": clip,
        "tm": tm,
        "core": core,
        "partner": clip + 1 - 2 * core,
        "i1": x * (1 - core) + y * core,
        "i2": y * (1 - core) + x * core,
        "s1": 1 + 3 * core,
        "s2": 4 - 3 * core,
    }
    spatial = Gather(sproj, proj_s, place, send_sem.at[0], recv_s)
    qkv = Gather(tqkv, qkv_w, place, send_sem.at[1], recv_q)
    temporal = Gather(tproj, proj_t, place, send_sem.at[2], recv_t)

    loads = [
        pltpu.make_async_copy(src, dst, local_sem.at[n])
        for n, (src, dst) in enumerate(
            [
                (sq, qkv_v.at[:, pl.ds(0, head_width)]),
                (sk, qkv_v.at[:, pl.ds(head_width, head_width)]),
                (sv, qkv_v.at[:, pl.ds(2 * head_width, head_width)]),
                (tokens, tok_v),
                (sproj, proj_s.at[tm]), (tqkv, qkv_w.at[tm]), (tproj, proj_t.at[tm]), (mask, mask_v),
                (ids, ids_v), (gates, gates_v), (w_gate, gate_w), (w_up, up_w), (w_down, down_w),
            ]
        )
    ]
    for load in loads[:10]:
        load.start()

    barrier = pltpu.get_barrier_semaphore()

    def greet(step, carry):
        other = lax.rem(me + step, DEVICES)
        pl.semaphore_signal(
            barrier, inc=1, device_id=(other // TM, lax.rem(other, TM)), device_id_type=MESH
        )
        return carry

    lax.fori_loop(1, DEVICES, greet, 0)
    pl.semaphore_wait(barrier, DEVICES - 1)

    spatial.own()
    qkv.own()

    for n in (0, 1, 2):
        loads[n].wait()
    triple_of = [qkv_v.at[:, pl.ds(n * head_width, head_width)] for n in range(3)]
    attend(*triple_of, mixed_v, None, HEADS)
    for load in loads[10:]:
        load.start()

    spatial.first_near()
    spatial.first_far()
    qkv.first_near()
    temporal.own()
    for k in range(4):
        spatial.second_near(k)
    for k in range(4):
        spatial.second_far(k)
    qkv.first_far()
    loads[3].wait()
    loads[4].wait()
    spatial.pushed()

    model = tok_v.shape[1]
    width = 512

    def project(chunk, carry):
        cols = pl.ds(pl.multiple_of(chunk * width, width), width)
        weights = proj_s[:, :, cols].reshape(mixed_v.shape[1], width)
        update = jnp.dot(mixed_v[...], weights, preferred_element_type=jnp.float32)
        tok_v[:, cols] = (tok_v[:, cols].astype(jnp.float32) + update).astype(jnp.bfloat16)
        return carry

    lax.fori_loop(0, model // width, project, 0)
    normed_rows(tok_v, normed_v)

    def swap(src_of, dst, slot):
        def step(shift, carry):
            other = lax.rem(tm + shift, TM)
            pltpu.make_async_remote_copy(
                src_ref=src_of(other),
                dst_ref=dst.at[tm],
                send_sem=swap_send.at[slot],
                recv_sem=swap_recv.at[slot],
                device_id=(clip, other),
                device_id_type=MESH,
            ).start()
            return carry

        lax.fori_loop(1, TM, step, 0)
        kept = pltpu.make_async_copy(src_of(tm), dst.at[tm], local_sem.at[13 + slot])
        kept.start()
        return kept

    def swapped(dst, kept, slot):
        ref = dst.at[pl.ds(0, TM - 1)]
        pltpu.make_async_copy(ref, ref, swap_recv.at[slot]).wait()
        kept.wait()

    def block_of(ref):
        return lambda index: ref.at[pl.ds(pl.multiple_of(index * per, per), per)]

    kept = swap(block_of(normed_v), spread_v, 0)

    temporal.first_near()
    for k in range(4):
        qkv.second_near(k)
    temporal.first_far()
    for k in range(4):
        qkv.second_far(k)

    rows = lax.broadcasted_iota(jnp.int32, (positions, TM), 0) // per
    cols16 = lax.broadcasted_iota(jnp.int32, (positions, TM), 1)
    frame_of = (rows == cols16).astype(jnp.float32)
    loads[7].wait()
    mask_f = jnp.where(mask_v[...] == 1, 1.0, 0.0)
    by_row = jnp.dot(frame_of, mask_f, preferred_element_type=jnp.float32)
    pairs = lax.dot_general(by_row, frame_of, (((1,), (1,)), ((), ())), preferred_element_type=jnp.float32)
    pos_r = lax.rem(lax.broadcasted_iota(jnp.int32, (positions, positions), 0), per)
    pos_c = lax.rem(lax.broadcasted_iota(jnp.int32, (positions, positions), 1), per)
    allowed_v[...] = jnp.where(pos_r == pos_c, pairs, 0.0)

    number_slots(ids_v, slots_v, slots_t, loads[8], clip, tm)

    loads[5].wait()
    qkv.pushed()
    swapped(spread_v, kept, 0)

    def triple(chunk):
        cols = pl.ds(chunk * width, width)
        weights = qkv_w[:, :, cols].reshape(model, width)
        rows_in = spread_v[...].reshape(positions, model)
        qkv_v[:, cols] = jnp.dot(rows_in, weights, preferred_element_type=jnp.float32).astype(jnp.bfloat16)

    for chunk in range(3 * head_width // width):
        triple(chunk)
        if chunk < 4:
            temporal.second_near(chunk)

    attend(*triple_of, mixed_v, allowed_v, HEADS)
    kept = swap(block_of(mixed_v), home_v, 1)
    for k in range(4):
        temporal.second_far(k)
    loads[6].wait()
    temporal.pushed()
    swapped(home_v, kept, 1)

    def finish(chunk, carry):
        cols = pl.ds(pl.multiple_of(chunk * width, width), width)
        weights = proj_t[:, :, cols].reshape(head_width, width)
        rows_in = home_v[...].reshape(positions, head_width)
        update = jnp.dot(rows_in, weights, preferred_element_type=jnp.float32).astype(jnp.bfloat16)
        tok_v[:, cols] = (
            tok_v[:, cols].astype(jnp.float32) + update.astype(jnp.float32)
        ).astype(jnp.bfloat16)
        return carry

    lax.fori_loop(0, model // width, finish, 0)
    ref = normed_v.at[pl.ds(0, positions - per)]
    pltpu.make_async_copy(ref, ref, swap_send.at[0]).wait()
    normed_rows(tok_v, normed_v)

    size = DEVICES // GROUPS
    slots = size * CAP

    def peer(order, sign):
        offset = lax.rem(order * STRIDE, DEVICES)
        dz, dc = lax.rem(offset, 4), lax.rem(offset // 4, 2)
        dy, dx = lax.rem(offset // 8, 4), offset // 32
        to_z = lax.rem(clip // 2 + sign * dz + 4, 4)
        to_c = lax.rem(core + dc, 2)
        to_y = lax.rem(y + sign * dy + 4, 4)
        to_x = lax.rem(x + sign * dx + 4, 4)
        return to_z * 2 + to_c, to_y * 4 + to_x

    def ship(group, sign, src, dst, sends, receives):
        def step(order, carry):
            to_clip, to_tm = peer(order, sign)

            @pl.when(order > 0)
            def _():
                pltpu.make_async_remote_copy(
                    src_ref=src.at[order],
                    dst_ref=dst.at[order],
                    send_sem=sends,
                    recv_sem=receives.at[group],
                    device_id=(to_clip, to_tm),
                    device_id_type=MESH,
                ).start()

            return carry

        lax.fori_loop(group * size, group * size + size, step, 0)

    def landed(group, dst, receives):
        ref = dst.at[pl.ds(0, size)]
        pltpu.make_async_copy(ref, ref, receives.at[group]).wait()

    def pick(group, table):
        return (lax.broadcasted_iota(jnp.int32, (slots, positions), 0) + group * slots == table).astype(
            jnp.float32
        )

    def build(group, carry):
        chosen = pick(group, slots_t[0:1, :]) + pick(group, slots_t[1:2, :])
        chosen = chosen.astype(jnp.bfloat16)
        for chunk in range(model // width):
            cols = pl.ds(chunk * width, width)
            rows_out = jnp.dot(chosen, normed_v[:, cols], preferred_element_type=jnp.float32)
            outgoing[pl.ds(group * size, size), :, cols] = rows_out.reshape(size, CAP, width).astype(
                jnp.bfloat16
            )
        ship(group, 1, outgoing, received, moe_send.at[0], go_recv)
        return carry

    lax.fori_loop(0, GROUPS, build, 0)
    pltpu.make_async_copy(outgoing.at[0], received.at[0], go_recv.at[0]).start()
    for load in loads[9:]:
        load.wait()

    def serve(group, carry):
        landed(group, received, go_recv)
        mine = pl.ds(group * size, size)
        for chunk in range(model // width):
            cols = pl.ds(chunk * width, width)
            wide = received[mine, :, cols].astype(jnp.float32)
            normed_v[:, cols] = wide.reshape(slots, width).astype(jnp.bfloat16)

        def gate_up(cols):
            rows_in = normed_v[...]
            gate_part = jnp.dot(rows_in, gate_w[:, cols], preferred_element_type=jnp.float32)
            up_part = jnp.dot(rows_in, up_w[:, cols], preferred_element_type=jnp.float32)
            hidden_v[:, cols] = (gate_part / (1.0 + jnp.exp(-gate_part)) * up_part).astype(jnp.bfloat16)

        def gate_step(chunk, carry):
            gate_up(pl.ds(pl.multiple_of(chunk * 256, 256), 256))
            return carry

        hidden = hidden_v.shape[1]
        lax.fori_loop(0, hidden // 256, gate_step, 0)
        if hidden % 256:
            gate_up(pl.ds(hidden - hidden % 256, hidden % 256))

        def down_step(chunk, carry):
            cols = pl.ds(pl.multiple_of(chunk * width, width), width)
            answer = jnp.dot(hidden_v[...], down_w[:, cols], preferred_element_type=jnp.float32)
            received[mine, :, cols] = answer.reshape(size, CAP, width).astype(jnp.bfloat16)
            return carry

        lax.fori_loop(0, model // width, down_step, 0)
        ship(group, -1, received, answers, moe_send.at[1], back_recv)

        @pl.when(group == 0)
        def _():
            pltpu.make_async_copy(received.at[0], answers.at[0], back_recv.at[0]).start()

        return carry

    lax.fori_loop(0, GROUPS, serve, 0)

    def combine(group, carry):
        landed(group, answers, back_recv)
        lanes = lax.broadcasted_iota(jnp.int32, (positions, slots), 1) + group * slots
        picks = [
            (lanes == slots_v[:, k : k + 1]).astype(jnp.float32).astype(jnp.bfloat16) for k in range(TOP)
        ]
        for chunk in range(model // width):
            cols = pl.ds(chunk * width, width)
            wide = answers[pl.ds(group * size, size), :, cols].astype(jnp.float32)
            rows_in = wide.reshape(slots, width).astype(jnp.bfloat16)
            parts = [
                jnp.dot(picks[k], rows_in, preferred_element_type=jnp.float32) * gates_v[:, k : k + 1]
                for k in range(TOP)
            ]
            part = parts[0] + parts[1]

            @pl.when(group == 0)
            def _():
                total_v[:, cols] = part

            @pl.when(group > 0)
            def _():
                total_v[:, cols] = total_v[:, cols] + part

        return carry

    lax.fori_loop(0, GROUPS, combine, 0)

    def close(block, carry):
        rows_at = pl.ds(pl.multiple_of(block * 32, 32), 32)
        tok_v[rows_at, :] = (tok_v[rows_at, :].astype(jnp.float32) + total_v[rows_at, :]).astype(jnp.bfloat16)
        return carry

    lax.fori_loop(0, positions // 32, close, 0)
    put = pltpu.make_async_copy(tok_v, out, local_sem.at[15])
    put.start()
    ref = mixed_v.at[pl.ds(0, positions - per)]
    pltpu.make_async_copy(ref, ref, swap_send.at[1]).wait()
    spatial.drained()
    qkv.drained()
    temporal.drained()
    ref = outgoing.at[pl.ds(0, DEVICES - 1)]
    pltpu.make_async_copy(ref, ref, moe_send.at[0]).wait()
    pltpu.make_async_copy(ref, ref, moe_send.at[1]).wait()
    put.wait()


def number_slots(ids_v, slots_v, slots_t, load, clip, tm):
    load.wait()
    positions = ids_v.shape[0]
    expert = lax.broadcasted_iota(jnp.int32, (positions, DEVICES), 1)
    e_clip, e_tm = expert // TM, lax.rem(expert, TM)
    dz = lax.rem(e_clip // 2 - clip // 2 + 4, 4)
    dc = lax.rem(lax.rem(e_clip, 2) - lax.rem(clip, 2) + 2, 2)
    dy = lax.rem(e_tm // SIDE - tm // SIDE + 4, 4)
    dx = lax.rem(lax.rem(e_tm, SIDE) - lax.rem(tm, SIDE) + 4, 4)
    order = lax.rem((dz + 4 * dc + 8 * dy + 32 * dx) * INVERSE, DEVICES)
    named = [(ids_v[:, k : k + 1] == expert).astype(jnp.float32) for k in range(TOP)]
    rows = lax.broadcasted_iota(jnp.int32, (positions, positions), 0)
    cols = lax.broadcasted_iota(jnp.int32, (positions, positions), 1)
    before = (cols < rows).astype(jnp.float32).astype(jnp.bfloat16)
    counts = jnp.dot(before, (named[0] + named[1]).astype(jnp.bfloat16), preferred_element_type=jnp.float32)
    row = (order * CAP).astype(jnp.float32) + counts
    found = [jnp.sum(named[k] * row, axis=1, keepdims=True) for k in range(TOP)]
    table = jnp.where(expert == 0, found[0], jnp.where(expert == 1, found[1], -1.0))
    slots_v[...] = table.astype(jnp.int32)
    slots_t[...] = table.T.astype(jnp.int32)


def layer(tokens, sq, sk, sv, sproj, tqkv, tproj, mask, ids, gates, w_gate, w_up, w_down):
    positions, model = tokens.shape
    head_width = sq.shape[1]
    per = positions // TM
    hidden = w_gate.shape[1]
    bf16 = jnp.bfloat16
    vm = lambda *shape: pltpu.VMEM(shape, bf16)
    dma = lambda n: pltpu.SemaphoreType.DMA((n,))
    any_spec = pl.BlockSpec(memory_space=pl.ANY)
    return pl.pallas_call(
        layer_kernel,
        out_shape=jax.ShapeDtypeStruct((positions, model), bf16),
        in_specs=[any_spec] * 13,
        out_specs=any_spec,
        scratch_shapes=[
            vm(positions, model), vm(positions, head_width), vm(positions, model), vm(TM, per, model),
            vm(positions, 3 * head_width), vm(TM, per, head_width),
            pltpu.VMEM((positions, positions), jnp.float32), pltpu.VMEM((TM, TM), jnp.int32),
            pltpu.VMEM((positions, TOP), jnp.int32), pltpu.VMEM((positions, TOP), jnp.float32),
            vm(TM, sproj.shape[0], model), vm(TM, tqkv.shape[0], 3 * head_width), vm(TM, tproj.shape[0], model),
            vm(model, hidden), vm(model, hidden), vm(hidden, model),
            vm(DEVICES, CAP, model), vm(DEVICES, CAP, model), vm(DEVICES, CAP, model),
            vm(positions, hidden), pltpu.VMEM((positions, model), jnp.float32),
            pltpu.VMEM((positions, DEVICES), jnp.int32), pltpu.VMEM((DEVICES, positions), jnp.int32),
            dma(16), dma(3), dma(21), dma(21), dma(21), dma(2), dma(2), dma(2), dma(GROUPS), dma(GROUPS),
        ],
        compiler_params=pltpu.CompilerParams(
            collective_id=0, has_side_effects=True, vmem_limit_bytes=67043328
        ),
        name="layer",
    )(tokens, sq, sk, sv, sproj, tqkv, tproj, mask, ids, gates, w_gate, w_up, w_down)


def shards(
    tokens,
    spatial_queries,
    spatial_keys,
    spatial_values,
    spatial_proj,
    temporal_qkv,
    temporal_proj,
    frame_mask,
    expert_ids,
    gate_values,
    expert_gate,
    expert_up,
    expert_down,
):
    positions, model_width = tokens.shape[2:]
    layer_out = layer(
        tokens.reshape(positions, model_width),
        spatial_queries.reshape(positions, -1),
        spatial_keys.reshape(positions, -1),
        spatial_values.reshape(positions, -1),
        spatial_proj,
        temporal_qkv,
        temporal_proj,
        frame_mask.reshape(frame_mask.shape[1:]),
        expert_ids.reshape(positions, TOP),
        gate_values.reshape(positions, TOP),
        expert_gate[0],
        expert_up[0],
        expert_down[0],
    )
    return layer_out.reshape(tokens.shape)


def solution(mesh):
    placed = (
        P("clip", "tm", None, None),
        P("clip", "tm", None, None),
        P("clip", "tm", None, None),
        P("clip", "tm", None, None),
        P("tm", None),
        P("tm", None),
        P("tm", None),
        P("clip", None, None),
        P("clip", "tm", None, None),
        P("clip", "tm", None, None),
        P(("clip", "tm"), None, None),
        P(("clip", "tm"), None, None),
        P(("clip", "tm"), None, None),
    )
    return jax.shard_map(
        shards, mesh=mesh, in_specs=placed, out_specs=P("clip", "tm", None, None), check_vma=False
    )
```

```python
import math

import jax
import jax.numpy as jnp
from jax import lax
from jax.experimental import pallas as pl
from jax.experimental.pallas import tpu as pltpu
from jax.sharding import PartitionSpec as P

HEADS = 8
HD = 128
TOP = 2
CAP = 8
SIDE = 4
TM = 16


EPS = 1e-06
MASKED = -1e30
MESH = pl.DeviceIdType.MESH
STRIDE = 49
INVERSE = pow(STRIDE, -1, 128)
GROUPS = 4
DEVICES = 128


class Gather:
    OFFSETS = (0, -1, 1, 2)
    EVENTS = ((-1, 0), (1, 0), (2, 0)) + tuple((i, j) for i in (0, -1, 1, 2) for j in (-1, 1)) + tuple(
        (i, 2) for i in (0, -1, 1, 2)
    )

    def __init__(self, shard, full, start, columns, place, send, recv, split):
        self.shard, self.full, self.send, self.recv = shard, full, send, recv
        self.start, self.columns, self.place, self.split = start, columns, place, split
        self.rows = full.shape[1]
        self.size = self.rows // 4 if split else self.rows // 2
        if split:
            self.base = place["parity"] * (self.rows // 2) + place["core"] * self.size
            self.other = (1 - place["parity"]) * (self.rows // 2) + place["core"] * self.size
        else:
            self.base = place["core"] * self.size

    def span(self, part):
        if part is None:
            return pl.ds(self.start, self.columns)
        return pl.ds(self.start + part * (self.columns // 2), self.columns // 2)

    def part(self, index, part=None, base=None):
        base = self.base if base is None else base
        return self.full.at[index, pl.ds(pl.multiple_of(base, self.size), self.size), self.span(part)]

    def own_part(self):
        return self.shard.at[pl.ds(pl.multiple_of(self.base, self.size), self.size), self.span(None)]

    def at(self, step1, step2):
        p = self.place
        return lax.rem(p["i1"] + step1 + SIDE, SIDE) * p["s1"] + lax.rem(p["i2"] + step2 + SIDE, SIDE) * p["s2"]

    def copy(self, src, dst, slot, clip, tm):
        pltpu.make_async_remote_copy(
            src_ref=src,
            dst_ref=dst,
            send_sem=self.send,
            recv_sem=self.recv.at[slot],
            device_id=(clip, tm),
            device_id_type=MESH,
        ).start()

    def arrived(self, ref, slot):
        pltpu.make_async_copy(ref, ref, self.recv.at[slot]).wait()

    def along(self, dim, way, src, dst, slot):
        target = self.at(way, 0) if dim == 1 else self.at(0, way)
        self.copy(src, dst, slot, self.place["clip"], target)

    def share(self, event):
        index = self.at(*self.EVENTS[event])
        whole = self.part(index)
        self.copy(whole, whole, 20, self.place["partner"], self.place["tm"])
        if self.split:
            for side in (0, 1):
                half = self.part(index, side)
                self.copy(half, half, 21 + event, self.place["above" if side == 0 else "below"], self.place["tm"])

    def lift(self, event):
        whole = self.part(self.at(*self.EVENTS[event]), base=self.other)
        self.arrived(whole, 21 + event)
        self.copy(whole, whole, 20, self.place["partner"], self.place["tm"])

    def second_dim(self, k):
        index = self.at(self.OFFSETS[k], 0)
        src = self.own_part() if k == 0 else self.part(index)
        self.along(2, 1, src, self.part(index), 4 + 2 * k)
        self.along(2, -1, src, self.part(index), 5 + 2 * k)
        if k > 0:
            self.share(k - 1)

    def own(self):
        mine = self.part(self.place["tm"])
        self.along(1, 1, self.own_part(), mine, 0)
        self.along(1, -1, self.own_part(), mine, 1)
        self.second_dim(0)

    def first_near(self):
        low, high = self.at(-1, 0), self.at(1, 0)
        self.arrived(self.part(low), 0)
        self.along(1, 1, self.part(low, 0), self.part(low, 0), 2)
        self.second_dim(1)
        self.arrived(self.part(high), 1)
        self.along(1, -1, self.part(high, 1), self.part(high, 1), 3)
        self.second_dim(2)

    def first_far(self):
        far = self.at(2, 0)
        self.arrived(self.part(far, 0), 2)
        self.arrived(self.part(far, 1), 3)
        self.second_dim(3)

    def second_near(self, k):
        step = self.OFFSETS[k]
        low, high = self.at(step, -1), self.at(step, 1)
        self.arrived(self.part(low), 4 + 2 * k)
        self.along(2, 1, self.part(low, 0), self.part(low, 0), 12 + 2 * k)
        self.share(3 + 2 * k)
        self.arrived(self.part(high), 5 + 2 * k)
        self.along(2, -1, self.part(high, 1), self.part(high, 1), 13 + 2 * k)
        self.share(4 + 2 * k)

    def second_far(self, k):
        far = self.at(self.OFFSETS[k], 2)
        self.arrived(self.part(far, 0), 12 + 2 * k)
        self.arrived(self.part(far, 1), 13 + 2 * k)
        self.share(11 + k)

    def pushed(self):
        self.arrived(self.full.at[pl.ds(0, TM - 1), pl.ds(0, self.rows // 2), self.span(None)], 20)

    def drained(self):
        ref = self.full.at[pl.ds(0, TM - 1), :, self.span(None)]
        pltpu.make_async_copy(ref, ref, self.send).wait()


def normed_rows(ref, out):
    def step(block, carry):
        rows = pl.ds(pl.multiple_of(block * 32, 32), 32)
        wide = ref[rows, :].astype(jnp.float32)
        inverse = lax.rsqrt(jnp.mean(wide * wide, axis=-1, keepdims=True) + EPS)
        out[rows, :] = (wide * inverse).astype(jnp.bfloat16)
        return carry

    lax.fori_loop(0, ref.shape[0] // 32, step, 0)


def head_weights(queries, keys, head, bias):
    cols = pl.ds(pl.multiple_of(head * HD, HD), HD)
    scores = lax.dot_general(
        queries[:, cols], keys[:, cols], (((1,), (1,)), ((), ())), preferred_element_type=jnp.float32
    )
    scores = scores * (1.0 / math.sqrt(HD))
    if bias is not None:
        scores = jnp.where(bias[...] > 0.5, scores, MASKED)
    terms = jnp.exp(scores - jnp.max(scores, axis=-1, keepdims=True))
    return (terms * (1.0 / jnp.sum(terms, axis=-1, keepdims=True))).astype(jnp.bfloat16)


def head_mix(weights, values, out, head):
    cols = pl.ds(pl.multiple_of(head * HD, HD), HD)
    mixed = jnp.dot(weights, values[:, cols], preferred_element_type=jnp.float32)
    out[:, cols] = mixed.astype(jnp.bfloat16)


def layer_kernel(
    tokens, sq, sk, sv, sproj, tqkv, tproj, mask, ids, gates, w_gate, w_up, w_down,
    out,
    tok_v, mixed_v, normed_v, spread_v, qkv_v, home_v, allowed_v, mask_v, ids_v, gates_v,
    proj_s, qkv_w, proj_t, gate_w, up_w, down_w, outgoing, received, answers, hidden_v, total_v,
    cols_v, slots_t, weights_v,
    local_sem, send_sem, recv_s, recv_q, recv_v, recv_t, swap_send, swap_recv, moe_send, go_recv, back_recv,
):
    clip = lax.axis_index("clip")
    tm = lax.axis_index("tm")
    core = lax.rem(clip, 2)
    y, x = tm // SIDE, lax.rem(tm, SIDE)
    positions = tok_v.shape[0]
    per = positions // TM
    head_width = HEADS * HD
    me = clip * TM + tm
    place = {
        "clip": clip,
        "tm": tm,
        "core": core,
        "partner": clip + 1 - 2 * core,
        "i1": x * (1 - core) + y * core,
        "i2": y * (1 - core) + x * core,
        "s1": 1 + 3 * core,
        "s2": 4 - 3 * core,
        "parity": lax.rem(clip // 2, 2),
        "above": lax.rem(clip + 2, DEVICES // TM),
        "below": lax.rem(clip + DEVICES // TM - 2, DEVICES // TM),
    }
    model = tok_v.shape[1]
    width = 512
    spatial = Gather(sproj, proj_s, 0, model, place, send_sem.at[0], recv_s, False)
    scored = Gather(tqkv, qkv_w, 0, 2 * head_width, place, send_sem.at[1], recv_q, True)
    valued = Gather(tqkv, qkv_w, 2 * head_width, head_width, place, send_sem.at[2], recv_v, True)
    temporal = Gather(tproj, proj_t, 0, model, place, send_sem.at[3], recv_t, True)

    loads = [
        pltpu.make_async_copy(src, dst, local_sem.at[n])
        for n, (src, dst) in enumerate(
            [
                (sq, qkv_v.at[:, pl.ds(0, head_width)]),
                (sk, qkv_v.at[:, pl.ds(head_width, head_width)]),
                (sv, qkv_v.at[:, pl.ds(2 * head_width, head_width)]),
                (tokens, tok_v),
                (sproj, proj_s.at[tm]), (tqkv, qkv_w.at[tm]), (tproj, proj_t.at[tm]), (mask, mask_v),
                (ids, ids_v), (gates, gates_v), (w_gate, gate_w), (w_up, up_w), (w_down, down_w),
            ]
        )
    ]
    for load in loads[:10]:
        load.start()

    barrier = pltpu.get_barrier_semaphore()

    def greet(step, carry):
        other = lax.rem(me + step, DEVICES)
        pl.semaphore_signal(
            barrier, inc=1, device_id=(other // TM, lax.rem(other, TM)), device_id_type=MESH
        )
        return carry

    lax.fori_loop(1, DEVICES, greet, 0)
    pl.semaphore_wait(barrier, DEVICES - 1)

    spatial.own()
    scored.own()

    for n in (0, 1, 2):
        loads[n].wait()
    triple_of = [qkv_v.at[:, pl.ds(n * head_width, head_width)] for n in range(3)]

    def mix_space(index, carry):
        for head in (2 * index, 2 * index + 1):
            head_mix(head_weights(triple_of[0], triple_of[1], head, None), triple_of[2], mixed_v, head)
        return carry

    lax.fori_loop(0, HEADS // 2, mix_space, 0)
    for load in loads[10:]:
        load.start()

    spatial.first_near()
    spatial.first_far()
    scored.first_near()
    for k in range(4):
        spatial.second_near(k)
    scored.first_far()
    for k in range(4):
        spatial.second_far(k)
    valued.own()
    loads[3].wait()
    loads[4].wait()
    spatial.pushed()

    def project(chunk, carry):
        cols = pl.ds(pl.multiple_of(chunk * width, width), width)
        weights = proj_s[:, :, cols].reshape(mixed_v.shape[1], width)
        update = jnp.dot(mixed_v[...], weights, preferred_element_type=jnp.float32)
        tok_v[:, cols] = (tok_v[:, cols].astype(jnp.float32) + update).astype(jnp.bfloat16)
        return carry

    lax.fori_loop(0, model // width, project, 0)
    normed_rows(tok_v, normed_v)

    def swap(src_of, dst, slot):
        def step(shift, carry):
            other = lax.rem(tm + shift, TM)
            pltpu.make_async_remote_copy(
                src_ref=src_of(other),
                dst_ref=dst.at[tm],
                send_sem=swap_send.at[slot],
                recv_sem=swap_recv.at[slot],
                device_id=(clip, other),
                device_id_type=MESH,
            ).start()
            return carry

        lax.fori_loop(1, TM, step, 0)
        kept = pltpu.make_async_copy(src_of(tm), dst.at[tm], local_sem.at[13 + slot])
        kept.start()
        return kept

    def swapped(dst, kept, slot):
        ref = dst.at[pl.ds(0, TM - 1)]
        pltpu.make_async_copy(ref, ref, swap_recv.at[slot]).wait()
        kept.wait()

    def block_of(ref):
        return lambda index: ref.at[pl.ds(pl.multiple_of(index * per, per), per)]

    kept = swap(block_of(normed_v), spread_v, 0)

    for event in (0, 1, 2):
        scored.lift(event)
    for k in range(4):
        scored.second_near(k)
    valued.first_near()
    valued.first_far()
    for k in range(4):
        scored.second_far(k)
    temporal.own()
    for event in range(3, 15):
        scored.lift(event)

    rows = lax.broadcasted_iota(jnp.int32, (positions, TM), 0) // per
    cols16 = lax.broadcasted_iota(jnp.int32, (positions, TM), 1)
    frame_of = (rows == cols16).astype(jnp.float32)
    loads[7].wait()
    mask_f = jnp.where(mask_v[...] == 1, 1.0, 0.0)
    by_row = jnp.dot(frame_of, mask_f, preferred_element_type=jnp.float32)
    pairs = lax.dot_general(by_row, frame_of, (((1,), (1,)), ((), ())), preferred_element_type=jnp.float32)
    pos_r = lax.rem(lax.broadcasted_iota(jnp.int32, (positions, positions), 0), per)
    pos_c = lax.rem(lax.broadcasted_iota(jnp.int32, (positions, positions), 1), per)
    allowed_v[...] = jnp.where(pos_r == pos_c, pairs, 0.0)

    number_slots(ids_v, gates_v, cols_v, slots_t, loads[8:10], clip, tm)

    loads[5].wait()
    scored.pushed()
    swapped(spread_v, kept, 0)

    def triple(chunk):
        cols = pl.ds(chunk * width, width)
        weights = qkv_w[:, :, cols].reshape(model, width)
        rows_in = spread_v[...].reshape(positions, model)
        qkv_v[:, cols] = jnp.dot(rows_in, weights, preferred_element_type=jnp.float32).astype(jnp.bfloat16)

    for chunk in range(2 * head_width // width):
        triple(chunk)
        valued.second_near(chunk)

    def weigh(index, carry):
        for head in (2 * index, 2 * index + 1):
            weights_v[head] = head_weights(triple_of[0], triple_of[1], head, allowed_v)
        return carry

    temporal.first_near()
    for event in (0, 1, 2, 3, 4):
        valued.lift(event)
    lax.fori_loop(0, HEADS // 4, weigh, 0)
    temporal.first_far()
    for k in range(4):
        valued.second_far(k)
    lax.fori_loop(HEADS // 4, HEADS // 2, weigh, 0)
    for event in range(5, 15):
        valued.lift(event)
    temporal.second_near(0)
    temporal.second_near(1)
    valued.pushed()
    for chunk in range(2 * head_width // width, 3 * head_width // width):
        triple(chunk)

    def mix_time(index, carry):
        for head in (2 * index, 2 * index + 1):
            head_mix(weights_v[head], triple_of[2], mixed_v, head)
        return carry

    lax.fori_loop(0, HEADS // 2, mix_time, 0)
    kept = swap(block_of(mixed_v), home_v, 1)
    temporal.second_near(2)
    temporal.second_near(3)
    for event in range(7):
        temporal.lift(event)
    for k in range(4):
        temporal.second_far(k)
    for event in range(7, 15):
        temporal.lift(event)
    loads[6].wait()
    temporal.pushed()
    swapped(home_v, kept, 1)

    def finish(chunk, carry):
        cols = pl.ds(pl.multiple_of(chunk * width, width), width)
        weights = proj_t[:, :, cols].reshape(head_width, width)
        rows_in = home_v[...].reshape(positions, head_width)
        update = jnp.dot(rows_in, weights, preferred_element_type=jnp.float32).astype(jnp.bfloat16)
        tok_v[:, cols] = (
            tok_v[:, cols].astype(jnp.float32) + update.astype(jnp.float32)
        ).astype(jnp.bfloat16)
        return carry

    lax.fori_loop(0, model // width, finish, 0)
    ref = normed_v.at[pl.ds(0, positions - per)]
    pltpu.make_async_copy(ref, ref, swap_send.at[0]).wait()
    normed_rows(tok_v, normed_v)

    size = DEVICES // GROUPS
    slots = size * CAP

    def peer(order, sign):
        offset = lax.rem(order * STRIDE, DEVICES)
        dz, dc = lax.rem(offset, 4), lax.rem(offset // 4, 2)
        dy, dx = lax.rem(offset // 8, 4), offset // 32
        to_z = lax.rem(clip // 2 + sign * dz + 4, 4)
        to_c = lax.rem(core + dc, 2)
        to_y = lax.rem(y + sign * dy + 4, 4)
        to_x = lax.rem(x + sign * dx + 4, 4)
        return to_z * 2 + to_c, to_y * 4 + to_x

    def ship(group, sign, src, dst, sends, receives):
        def step(order, carry):
            to_clip, to_tm = peer(order, sign)

            @pl.when(order > 0)
            def _():
                pltpu.make_async_remote_copy(
                    src_ref=src.at[order],
                    dst_ref=dst.at[order],
                    send_sem=sends,
                    recv_sem=receives.at[group],
                    device_id=(to_clip, to_tm),
                    device_id_type=MESH,
                ).start()

            return carry

        lax.fori_loop(group * size, group * size + size, step, 0)

    def landed(group, dst, receives):
        ref = dst.at[pl.ds(0, size)]
        pltpu.make_async_copy(ref, ref, receives.at[group]).wait()

    def pick(group, table):
        return (lax.broadcasted_iota(jnp.int32, (slots, positions), 0) + group * slots == table).astype(
            jnp.float32
        )

    def build(group, carry):
        chosen = pick(group, slots_t[0:1, :]) + pick(group, slots_t[1:2, :])
        chosen = chosen.astype(jnp.bfloat16)
        for chunk in range(model // width):
            cols = pl.ds(chunk * width, width)
            rows_out = jnp.dot(chosen, normed_v[:, cols], preferred_element_type=jnp.float32)
            outgoing[pl.ds(group * size, size), :, cols] = rows_out.reshape(size, CAP, width).astype(
                jnp.bfloat16
            )
        ship(group, 1, outgoing, received, moe_send.at[0], go_recv)
        return carry

    lax.fori_loop(0, GROUPS, build, 0)
    pltpu.make_async_copy(outgoing.at[0], received.at[0], go_recv.at[0]).start()
    for load in loads[10:]:
        load.wait()

    def serve(group, carry):
        landed(group, received, go_recv)
        mine = pl.ds(group * size, size)
        for chunk in range(model // width):
            cols = pl.ds(chunk * width, width)
            wide = received[mine, :, cols].astype(jnp.float32)
            normed_v[:, cols] = wide.reshape(slots, width).astype(jnp.bfloat16)

        def gate_up(cols):
            rows_in = normed_v[...]
            gate_part = jnp.dot(rows_in, gate_w[:, cols], preferred_element_type=jnp.float32)
            up_part = jnp.dot(rows_in, up_w[:, cols], preferred_element_type=jnp.float32)
            hidden_v[:, cols] = (gate_part / (1.0 + jnp.exp(-gate_part)) * up_part).astype(jnp.bfloat16)

        def gate_step(chunk, carry):
            gate_up(pl.ds(pl.multiple_of(chunk * 256, 256), 256))
            return carry

        hidden = hidden_v.shape[1]
        lax.fori_loop(0, hidden // 256, gate_step, 0)
        if hidden % 256:
            gate_up(pl.ds(hidden - hidden % 256, hidden % 256))

        def down_step(chunk, carry):
            cols = pl.ds(pl.multiple_of(chunk * width, width), width)
            answer = jnp.dot(hidden_v[...], down_w[:, cols], preferred_element_type=jnp.float32)
            received[mine, :, cols] = answer.reshape(size, CAP, width).astype(jnp.bfloat16)
            return carry

        lax.fori_loop(0, model // width, down_step, 0)
        ship(group, -1, received, answers, moe_send.at[1], back_recv)

        @pl.when(group == 0)
        def _():
            pltpu.make_async_copy(received.at[0], answers.at[0], back_recv.at[0]).start()

        return carry

    lax.fori_loop(0, GROUPS, serve, 0)

    def combine(group, carry):
        landed(group, answers, back_recv)
        lanes = lax.broadcasted_iota(jnp.int32, (positions, slots), 1) + group * slots
        picks = [
            (lanes == cols_v[:, k : k + 1].astype(jnp.int32)).astype(jnp.float32).astype(jnp.bfloat16) for k in range(TOP)
        ]
        for chunk in range(model // width):
            cols = pl.ds(chunk * width, width)
            wide = answers[pl.ds(group * size, size), :, cols].astype(jnp.float32)
            rows_in = wide.reshape(slots, width).astype(jnp.bfloat16)
            parts = [
                jnp.dot(picks[k], rows_in, preferred_element_type=jnp.float32) * cols_v[:, TOP + k : TOP + k + 1]
                for k in range(TOP)
            ]
            part = parts[0] + parts[1]

            @pl.when(group == 0)
            def _():
                total_v[:, cols] = part

            @pl.when(group > 0)
            def _():
                total_v[:, cols] = total_v[:, cols] + part

        return carry

    lax.fori_loop(0, GROUPS, combine, 0)

    def close(block, carry):
        rows_at = pl.ds(pl.multiple_of(block * 32, 32), 32)
        tok_v[rows_at, :] = (tok_v[rows_at, :].astype(jnp.float32) + total_v[rows_at, :]).astype(jnp.bfloat16)
        return carry

    lax.fori_loop(0, positions // 32, close, 0)
    put = pltpu.make_async_copy(tok_v, out, local_sem.at[15])
    put.start()
    ref = mixed_v.at[pl.ds(0, positions - per)]
    pltpu.make_async_copy(ref, ref, swap_send.at[1]).wait()
    spatial.drained()
    scored.drained()
    valued.drained()
    temporal.drained()
    ref = outgoing.at[pl.ds(0, DEVICES - 1)]
    pltpu.make_async_copy(ref, ref, moe_send.at[0]).wait()
    pltpu.make_async_copy(ref, ref, moe_send.at[1]).wait()
    put.wait()


def number_slots(ids_v, gates_v, cols_v, slots_t, loads, clip, tm):
    for load in loads:
        load.wait()
    positions = ids_v.shape[1]
    expert = lax.broadcasted_iota(jnp.int32, (DEVICES, positions), 0)
    e_clip, e_tm = expert // TM, lax.rem(expert, TM)
    dz = lax.rem(e_clip // 2 - clip // 2 + 4, 4)
    dc = lax.rem(lax.rem(e_clip, 2) - lax.rem(clip, 2) + 2, 2)
    dy = lax.rem(e_tm // SIDE - tm // SIDE + 4, 4)
    dx = lax.rem(lax.rem(e_tm, SIDE) - lax.rem(tm, SIDE) + 4, 4)
    order = lax.rem((dz + 4 * dc + 8 * dy + 32 * dx) * INVERSE, DEVICES)
    named = [(ids_v[k : k + 1, :] == expert).astype(jnp.float32) for k in range(TOP)]
    rows = lax.broadcasted_iota(jnp.int32, (positions, positions), 0)
    cols = lax.broadcasted_iota(jnp.int32, (positions, positions), 1)
    before = (rows < cols).astype(jnp.float32).astype(jnp.bfloat16)
    counts = jnp.dot((named[0] + named[1]).astype(jnp.bfloat16), before, preferred_element_type=jnp.float32)
    row = (order * CAP).astype(jnp.float32) + counts
    table = jnp.zeros((DEVICES, positions), jnp.float32)
    for k in range(TOP):
        found = jnp.sum(named[k] * row, axis=0, keepdims=True)
        slots_t[k : k + 1, :] = found.astype(jnp.int32)
        table = jnp.where(expert == k, found, table)
        table = jnp.where(expert == TOP + k, gates_v[k : k + 1, :], table)
    cols_v[...] = table.T


def layer(tokens, sq, sk, sv, sproj, tqkv, tproj, mask, ids, gates, w_gate, w_up, w_down):
    positions, model = tokens.shape
    head_width = sq.shape[1]
    per = positions // TM
    hidden = w_gate.shape[1]
    bf16 = jnp.bfloat16
    vm = lambda *shape: pltpu.VMEM(shape, bf16)
    dma = lambda n: pltpu.SemaphoreType.DMA((n,))
    any_spec = pl.BlockSpec(memory_space=pl.ANY)
    return pl.pallas_call(
        layer_kernel,
        out_shape=jax.ShapeDtypeStruct((positions, model), bf16),
        in_specs=[any_spec] * 13,
        out_specs=any_spec,
        scratch_shapes=[
            vm(positions, model), vm(positions, head_width), vm(positions, model), vm(TM, per, model),
            vm(positions, 3 * head_width), vm(TM, per, head_width),
            pltpu.VMEM((positions, positions), jnp.float32), pltpu.VMEM((TM, TM), jnp.int32),
            pltpu.VMEM((TOP, positions), jnp.int32), pltpu.VMEM((TOP, positions), jnp.float32),
            vm(TM, sproj.shape[0], model), vm(TM, tqkv.shape[0], 3 * head_width), vm(TM, tproj.shape[0], model),
            vm(model, hidden), vm(model, hidden), vm(hidden, model),
            vm(DEVICES, CAP, model), vm(DEVICES, CAP, model), vm(DEVICES, CAP, model),
            vm(positions, hidden), pltpu.VMEM((positions, model), jnp.float32),
            pltpu.VMEM((positions, DEVICES), jnp.float32), pltpu.VMEM((8, positions), jnp.int32),
            vm(HEADS, positions, positions),
            dma(16), dma(4), dma(36), dma(36), dma(36), dma(36), dma(2), dma(2), dma(2), dma(GROUPS), dma(GROUPS),
        ],
        compiler_params=pltpu.CompilerParams(
            collective_id=0, has_side_effects=True, vmem_limit_bytes=67043328
        ),
        name="layer",
    )(tokens, sq, sk, sv, sproj, tqkv, tproj, mask, ids, gates, w_gate, w_up, w_down)


def shards(
    tokens,
    spatial_queries,
    spatial_keys,
    spatial_values,
    spatial_proj,
    temporal_qkv,
    temporal_proj,
    frame_mask,
    expert_ids,
    gate_values,
    expert_gate,
    expert_up,
    expert_down,
):
    positions, model_width = tokens.shape[2:]
    layer_out = layer(
        tokens.reshape(positions, model_width),
        spatial_queries.reshape(positions, -1),
        spatial_keys.reshape(positions, -1),
        spatial_values.reshape(positions, -1),
        spatial_proj,
        temporal_qkv,
        temporal_proj,
        frame_mask.reshape(frame_mask.shape[1:]),
        expert_ids.reshape(positions, TOP).T,
        gate_values.reshape(positions, TOP).T,
        expert_gate[0],
        expert_up[0],
        expert_down[0],
    )
    return layer_out.reshape(tokens.shape)


def solution(mesh):
    placed = (
        P("clip", "tm", None, None),
        P("clip", "tm", None, None),
        P("clip", "tm", None, None),
        P("clip", "tm", None, None),
        P("tm", None),
        P("tm", None),
        P("tm", None),
        P("clip", None, None),
        P("clip", "tm", None, None),
        P("clip", "tm", None, None),
        P(("clip", "tm"), None, None),
        P(("clip", "tm"), None, None),
        P(("clip", "tm"), None, None),
    )
    return jax.shard_map(
        shards, mesh=mesh, in_specs=placed, out_specs=P("clip", "tm", None, None), check_vma=False
    )
```

```python
import math

import jax
import jax.numpy as jnp
from jax import lax
from jax.experimental import pallas as pl
from jax.experimental.pallas import tpu as pltpu
from jax.sharding import PartitionSpec as P

HEADS = 8
HD = 128
TOP = 2
CAP = 8
SIDE = 4
TM = 16


EPS = 1e-06
MASKED = -1e30
MESH = pl.DeviceIdType.MESH
STRIDE = 49
INVERSE = pow(STRIDE, -1, 128)
GROUPS = 4
DEVICES = 128


class Gather:
    OFFSETS = (0, -1, 1, 2)
    EVENTS = ((-1, 0), (1, 0), (2, 0)) + tuple((i, j) for i in (0, -1, 1, 2) for j in (-1, 1)) + tuple(
        (i, 2) for i in (0, -1, 1, 2)
    )

    def __init__(self, shard, full, start, columns, place, send, recv, split):
        self.shard, self.full, self.send, self.recv = shard, full, send, recv
        self.start, self.columns, self.place, self.split = start, columns, place, split
        self.rows = full.shape[1]
        self.size = self.rows // 4 if split else self.rows // 2
        if split:
            self.base = place["parity"] * (self.rows // 2) + place["core"] * self.size
            self.other = (1 - place["parity"]) * (self.rows // 2) + place["core"] * self.size
        else:
            self.base = place["core"] * self.size

    def span(self, part):
        if part is None:
            return pl.ds(self.start, self.columns)
        return pl.ds(self.start + part * (self.columns // 2), self.columns // 2)

    def part(self, index, part=None, base=None):
        base = self.base if base is None else base
        return self.full.at[index, pl.ds(pl.multiple_of(base, self.size), self.size), self.span(part)]

    def own_part(self):
        return self.shard.at[pl.ds(pl.multiple_of(self.base, self.size), self.size), self.span(None)]

    def at(self, step1, step2):
        p = self.place
        return lax.rem(p["i1"] + step1 + SIDE, SIDE) * p["s1"] + lax.rem(p["i2"] + step2 + SIDE, SIDE) * p["s2"]

    def copy(self, src, dst, slot, clip, tm):
        pltpu.make_async_remote_copy(
            src_ref=src,
            dst_ref=dst,
            send_sem=self.send,
            recv_sem=self.recv.at[slot],
            device_id=(clip, tm),
            device_id_type=MESH,
        ).start()

    def arrived(self, ref, slot):
        pltpu.make_async_copy(ref, ref, self.recv.at[slot]).wait()

    def along(self, dim, way, src, dst, slot):
        target = self.at(way, 0) if dim == 1 else self.at(0, way)
        self.copy(src, dst, slot, self.place["clip"], target)

    def share(self, event):
        index = self.at(*self.EVENTS[event])
        whole = self.part(index)
        self.copy(whole, whole, 20, self.place["partner"], self.place["tm"])
        if self.split:
            for side in (0, 1):
                half = self.part(index, side)
                self.copy(half, half, 21 + event, self.place["above" if side == 0 else "below"], self.place["tm"])

    def lift(self, event):
        whole = self.part(self.at(*self.EVENTS[event]), base=self.other)
        self.arrived(whole, 21 + event)
        self.copy(whole, whole, 20, self.place["partner"], self.place["tm"])

    def second_dim(self, k):
        index = self.at(self.OFFSETS[k], 0)
        src = self.own_part() if k == 0 else self.part(index)
        self.along(2, 1, src, self.part(index), 4 + 2 * k)
        self.along(2, -1, src, self.part(index), 5 + 2 * k)
        if k > 0:
            self.share(k - 1)

    def own(self):
        mine = self.part(self.place["tm"])
        self.along(1, 1, self.own_part(), mine, 0)
        self.along(1, -1, self.own_part(), mine, 1)
        self.second_dim(0)

    def first_near(self):
        low, high = self.at(-1, 0), self.at(1, 0)
        self.arrived(self.part(low), 0)
        self.along(1, 1, self.part(low, 0), self.part(low, 0), 2)
        self.second_dim(1)
        self.arrived(self.part(high), 1)
        self.along(1, -1, self.part(high, 1), self.part(high, 1), 3)
        self.second_dim(2)

    def first_far(self):
        far = self.at(2, 0)
        self.arrived(self.part(far, 0), 2)
        self.arrived(self.part(far, 1), 3)
        self.second_dim(3)

    def second_near(self, k):
        step = self.OFFSETS[k]
        low, high = self.at(step, -1), self.at(step, 1)
        self.arrived(self.part(low), 4 + 2 * k)
        self.along(2, 1, self.part(low, 0), self.part(low, 0), 12 + 2 * k)
        self.share(3 + 2 * k)
        self.arrived(self.part(high), 5 + 2 * k)
        self.along(2, -1, self.part(high, 1), self.part(high, 1), 13 + 2 * k)
        self.share(4 + 2 * k)

    def second_far(self, k):
        far = self.at(self.OFFSETS[k], 2)
        self.arrived(self.part(far, 0), 12 + 2 * k)
        self.arrived(self.part(far, 1), 13 + 2 * k)
        self.share(11 + k)

    def pushed(self):
        self.arrived(self.full.at[pl.ds(0, TM - 1), pl.ds(0, self.rows // 2), self.span(None)], 20)

    def drained(self):
        ref = self.full.at[pl.ds(0, TM - 1), :, self.span(None)]
        pltpu.make_async_copy(ref, ref, self.send).wait()


def normed_rows(ref, out):
    def step(block, carry):
        rows = pl.ds(pl.multiple_of(block * 32, 32), 32)
        wide = ref[rows, :].astype(jnp.float32)
        inverse = lax.rsqrt(jnp.mean(wide * wide, axis=-1, keepdims=True) + EPS)
        out[rows, :] = (wide * inverse).astype(jnp.bfloat16)
        return carry

    lax.fori_loop(0, ref.shape[0] // 32, step, 0)


def head_weights(queries, keys, head, bias):
    cols = pl.ds(pl.multiple_of(head * HD, HD), HD)
    scores = lax.dot_general(
        queries[:, cols], keys[:, cols], (((1,), (1,)), ((), ())), preferred_element_type=jnp.float32
    )
    scores = scores * (1.0 / math.sqrt(HD))
    if bias is not None:
        scores = jnp.where(bias[...] > 0.5, scores, MASKED)
    terms = jnp.exp(scores - jnp.max(scores, axis=-1, keepdims=True))
    return (terms * (1.0 / jnp.sum(terms, axis=-1, keepdims=True))).astype(jnp.bfloat16)


def head_mix(weights, values, out, head):
    cols = pl.ds(pl.multiple_of(head * HD, HD), HD)
    mixed = jnp.dot(weights, values[:, cols], preferred_element_type=jnp.float32)
    out[:, cols] = mixed.astype(jnp.bfloat16)


def layer_kernel(
    tokens, sq, sk, sv, sproj, tqkv, tproj, mask, ids, gates, w_gate, w_up, w_down,
    out,
    tok_v, mixed_v, normed_v, spread_v, qkv_v, home_v, allowed_v, mask_v, ids_v, gates_v,
    proj_s, qkv_w, proj_t, gate_w, up_w, down_w, outgoing, received, answers, hidden_v, total_v,
    cols_v, slots_t, weights_v,
    local_sem, send_sem, recv_s, recv_q, recv_v, recv_t, swap_send, swap_recv, moe_send, go_recv, back_recv,
):
    clip = lax.axis_index("clip")
    tm = lax.axis_index("tm")
    core = lax.rem(clip, 2)
    y, x = tm // SIDE, lax.rem(tm, SIDE)
    positions = tok_v.shape[0]
    per = positions // TM
    head_width = HEADS * HD
    me = clip * TM + tm
    place = {
        "clip": clip,
        "tm": tm,
        "core": core,
        "partner": clip + 1 - 2 * core,
        "i1": x * (1 - core) + y * core,
        "i2": y * (1 - core) + x * core,
        "s1": 1 + 3 * core,
        "s2": 4 - 3 * core,
        "parity": lax.rem(clip // 2, 2),
        "above": lax.rem(clip + 2, DEVICES // TM),
        "below": lax.rem(clip + DEVICES // TM - 2, DEVICES // TM),
    }
    model = tok_v.shape[1]
    width = 512
    spatial = Gather(sproj, proj_s, 0, model, place, send_sem.at[0], recv_s, False)
    scored = Gather(tqkv, qkv_w, 0, 2 * head_width, place, send_sem.at[1], recv_q, True)
    valued = Gather(tqkv, qkv_w, 2 * head_width, head_width, place, send_sem.at[2], recv_v, True)
    temporal = Gather(tproj, proj_t, 0, model, place, send_sem.at[3], recv_t, False)

    loads = [
        pltpu.make_async_copy(src, dst, local_sem.at[n])
        for n, (src, dst) in enumerate(
            [
                (sq, qkv_v.at[:, pl.ds(0, head_width)]),
                (sk, qkv_v.at[:, pl.ds(head_width, head_width)]),
                (sv, qkv_v.at[:, pl.ds(2 * head_width, head_width)]),
                (tokens, tok_v),
                (sproj, proj_s.at[tm]), (tqkv, qkv_w.at[tm]), (tproj, proj_t.at[tm]), (mask, mask_v),
                (ids, ids_v), (gates, gates_v), (w_gate, gate_w), (w_up, up_w), (w_down, down_w),
            ]
        )
    ]
    for load in loads[:10]:
        load.start()

    barrier = pltpu.get_barrier_semaphore()

    clips = [lax.rem(clip + n, DEVICES // TM) for n in range(DEVICES // TM)]
    tms = [lax.rem(tm + n, TM) for n in range(TM)]
    for n in range(1, DEVICES):
        pl.semaphore_signal(
            barrier, inc=1, device_id=(clips[n // TM], tms[n % TM]), device_id_type=MESH
        )
    pl.semaphore_wait(barrier, DEVICES - 1)

    spatial.own()
    scored.own()

    for n in (0, 1, 2):
        loads[n].wait()
    triple_of = [qkv_v.at[:, pl.ds(n * head_width, head_width)] for n in range(3)]

    def mix_space(index, carry):
        for head in (2 * index, 2 * index + 1):
            head_mix(head_weights(triple_of[0], triple_of[1], head, None), triple_of[2], mixed_v, head)
        return carry

    lax.fori_loop(0, HEADS // 2, mix_space, 0)
    for load in loads[10:]:
        load.start()

    spatial.first_near()
    spatial.second_near(0)
    scored.first_near()
    scored.second_near(0)
    spatial.first_far()
    spatial.second_near(1)
    scored.first_far()
    scored.lift(0)
    spatial.second_near(2)
    scored.lift(1)
    spatial.second_far(0)
    scored.lift(3)
    scored.second_near(1)
    valued.own()
    scored.lift(4)
    scored.second_near(2)
    scored.second_far(0)
    scored.lift(2)
    valued.first_near()
    scored.lift(5)
    spatial.second_near(3)
    spatial.second_far(1)
    scored.lift(6)
    valued.first_far()
    scored.second_near(3)
    scored.lift(7)
    spatial.second_far(2)
    scored.second_far(1)
    scored.lift(8)
    valued.second_near(0)
    scored.second_far(2)
    valued.second_near(1)
    valued.second_near(2)
    spatial.second_far(3)
    valued.second_near(3)
    temporal.own()
    loads[3].wait()
    loads[4].wait()
    spatial.pushed()

    def project(chunk, carry):
        cols = pl.ds(pl.multiple_of(chunk * width, width), width)
        weights = proj_s[:, :, cols].reshape(mixed_v.shape[1], width)
        update = jnp.dot(mixed_v[...], weights, preferred_element_type=jnp.float32)
        tok_v[:, cols] = (tok_v[:, cols].astype(jnp.float32) + update).astype(jnp.bfloat16)
        return carry

    lax.fori_loop(0, model // width, project, 0)
    normed_rows(tok_v, normed_v)

    def swap(src_of, dst, slot):
        def step(shift, carry):
            other = lax.rem(tm + shift, TM)
            pltpu.make_async_remote_copy(
                src_ref=src_of(other),
                dst_ref=dst.at[tm],
                send_sem=swap_send.at[slot],
                recv_sem=swap_recv.at[slot],
                device_id=(clip, other),
                device_id_type=MESH,
            ).start()
            return carry

        lax.fori_loop(1, TM, step, 0)
        kept = pltpu.make_async_copy(src_of(tm), dst.at[tm], local_sem.at[13 + slot])
        kept.start()
        return kept

    def swapped(dst, kept, slot):
        ref = dst.at[pl.ds(0, TM - 1)]
        pltpu.make_async_copy(ref, ref, swap_recv.at[slot]).wait()
        kept.wait()

    def block_of(ref):
        return lambda index: ref.at[pl.ds(pl.multiple_of(index * per, per), per)]

    kept = swap(block_of(normed_v), spread_v, 0)

    scored.second_far(3)
    for k in range(4):
        valued.second_far(k)
    for event in (11, 9, 10, 12):
        scored.lift(event)
    for event in (0, 1, 2):
        valued.lift(event)

    rows = lax.broadcasted_iota(jnp.int32, (positions, TM), 0) // per
    cols16 = lax.broadcasted_iota(jnp.int32, (positions, TM), 1)
    frame_of = (rows == cols16).astype(jnp.float32)
    loads[7].wait()
    mask_f = jnp.where(mask_v[...] == 1, 1.0, 0.0)
    by_row = jnp.dot(frame_of, mask_f, preferred_element_type=jnp.float32)
    pairs = lax.dot_general(by_row, frame_of, (((1,), (1,)), ((), ())), preferred_element_type=jnp.float32)
    pos_r = lax.rem(lax.broadcasted_iota(jnp.int32, (positions, positions), 0), per)
    pos_c = lax.rem(lax.broadcasted_iota(jnp.int32, (positions, positions), 1), per)
    allowed_v[...] = jnp.where(pos_r == pos_c, pairs, 0.0)

    number_slots(ids_v, gates_v, cols_v, slots_t, loads[8:10], clip, tm)

    temporal.first_near()
    temporal.second_near(0)
    valued.lift(3)
    valued.lift(4)
    scored.lift(13)
    for event in range(5, 11):
        valued.lift(event)
    scored.lift(14)
    for event in range(11, 15):
        valued.lift(event)
    loads[5].wait()
    scored.pushed()
    swapped(spread_v, kept, 0)

    def triple(chunk):
        cols = pl.ds(chunk * width, width)
        weights = qkv_w[:, :, cols].reshape(model, width)
        rows_in = spread_v[...].reshape(positions, model)
        qkv_v[:, cols] = jnp.dot(rows_in, weights, preferred_element_type=jnp.float32).astype(jnp.bfloat16)

    for chunk in range(2 * head_width // width):
        triple(chunk)
        if chunk == 2:
            temporal.first_far()
            temporal.second_near(1)

    def weigh(index, carry):
        for head in (2 * index, 2 * index + 1):
            weights_v[head] = head_weights(triple_of[0], triple_of[1], head, allowed_v)
        return carry

    lax.fori_loop(0, HEADS // 4, weigh, 0)
    temporal.second_near(2)
    lax.fori_loop(HEADS // 4, HEADS // 2, weigh, 0)
    temporal.second_far(0)
    valued.pushed()
    for chunk in range(2 * head_width // width, 3 * head_width // width):
        triple(chunk)
    temporal.second_far(1)
    temporal.second_near(3)

    def mix_time(index, carry):
        for head in (2 * index, 2 * index + 1):
            head_mix(weights_v[head], triple_of[2], mixed_v, head)
        return carry

    lax.fori_loop(0, HEADS // 2, mix_time, 0)
    kept = swap(block_of(mixed_v), home_v, 1)
    temporal.second_far(2)
    temporal.second_far(3)
    loads[6].wait()
    temporal.pushed()
    swapped(home_v, kept, 1)

    def finish(chunk, carry):
        cols = pl.ds(pl.multiple_of(chunk * width, width), width)
        weights = proj_t[:, :, cols].reshape(head_width, width)
        rows_in = home_v[...].reshape(positions, head_width)
        update = jnp.dot(rows_in, weights, preferred_element_type=jnp.float32).astype(jnp.bfloat16)
        tok_v[:, cols] = (
            tok_v[:, cols].astype(jnp.float32) + update.astype(jnp.float32)
        ).astype(jnp.bfloat16)
        return carry

    lax.fori_loop(0, model // width, finish, 0)
    ref = normed_v.at[pl.ds(0, positions - per)]
    pltpu.make_async_copy(ref, ref, swap_send.at[0]).wait()
    normed_rows(tok_v, normed_v)

    size = DEVICES // GROUPS
    slots = size * CAP

    def ship(group, sign, src, dst, sends, receives):
        to_clip = [
            lax.rem(clip // 2 + sign * dz + 4, 4) * 2 + lax.rem(core + dc, 2) for dc in range(2) for dz in range(4)
        ]
        to_y = [lax.rem(y + sign * dy + 4, 4) * 4 for dy in range(4)]
        to_x = [lax.rem(x + sign * (dx + group) + 8, 4) for dx in range(4)]
        to_tm = [row + col for col in to_x for row in to_y]

        def send(message, offset):
            pltpu.make_async_remote_copy(
                src_ref=src.at[group * size + message],
                dst_ref=dst.at[group * size + message],
                send_sem=sends,
                recv_sem=receives.at[group],
                device_id=(to_clip[offset % 8], to_tm[offset // 8]),
                device_id_type=MESH,
            ).start()

        @pl.when(group > 0)
        def _():
            send(0, 0)

        for message in range(1, size):
            send(message, message * STRIDE % DEVICES)

    def landed(group, dst, receives):
        ref = dst.at[pl.ds(0, size)]
        pltpu.make_async_copy(ref, ref, receives.at[group]).wait()

    def pick(group, table):
        return (lax.broadcasted_iota(jnp.int32, (slots, positions), 0) + group * slots == table).astype(
            jnp.float32
        )

    def build(group, carry):
        chosen = pick(group, slots_t[0:1, :]) + pick(group, slots_t[1:2, :])
        chosen = chosen.astype(jnp.bfloat16)
        for chunk in range(model // width):
            cols = pl.ds(chunk * width, width)
            rows_out = jnp.dot(chosen, normed_v[:, cols], preferred_element_type=jnp.float32)
            outgoing[pl.ds(group * size, size), :, cols] = rows_out.reshape(size, CAP, width).astype(
                jnp.bfloat16
            )
        ship(group, 1, outgoing, received, moe_send.at[0], go_recv)
        return carry

    lax.fori_loop(0, GROUPS, build, 0)
    pltpu.make_async_copy(outgoing.at[0], received.at[0], go_recv.at[0]).start()
    for load in loads[10:]:
        load.wait()

    def serve(group, carry):
        landed(group, received, go_recv)
        mine = pl.ds(group * size, size)
        for chunk in range(model // width):
            cols = pl.ds(chunk * width, width)
            wide = received[mine, :, cols].astype(jnp.float32)
            normed_v[:, cols] = wide.reshape(slots, width).astype(jnp.bfloat16)

        def gate_up(cols):
            rows_in = normed_v[...]
            gate_part = jnp.dot(rows_in, gate_w[:, cols], preferred_element_type=jnp.float32)
            up_part = jnp.dot(rows_in, up_w[:, cols], preferred_element_type=jnp.float32)
            hidden_v[:, cols] = (gate_part / (1.0 + jnp.exp(-gate_part)) * up_part).astype(jnp.bfloat16)

        def gate_step(chunk, carry):
            gate_up(pl.ds(pl.multiple_of(chunk * 256, 256), 256))
            return carry

        hidden = hidden_v.shape[1]
        lax.fori_loop(0, hidden // 256, gate_step, 0)
        if hidden % 256:
            gate_up(pl.ds(hidden - hidden % 256, hidden % 256))

        def down_step(chunk, carry):
            cols = pl.ds(pl.multiple_of(chunk * width, width), width)
            answer = jnp.dot(hidden_v[...], down_w[:, cols], preferred_element_type=jnp.float32)
            received[mine, :, cols] = answer.reshape(size, CAP, width).astype(jnp.bfloat16)
            return carry

        lax.fori_loop(0, model // width, down_step, 0)
        ship(group, -1, received, answers, moe_send.at[1], back_recv)

        @pl.when(group == 0)
        def _():
            pltpu.make_async_copy(received.at[0], answers.at[0], back_recv.at[0]).start()

        return carry

    lax.fori_loop(0, GROUPS, serve, 0)

    def answered(group, finish):
        landed(group, answers, back_recv)
        lanes = lax.broadcasted_iota(jnp.int32, (positions, slots), 1) + group * slots
        picks = [
            (lanes == cols_v[:, k : k + 1].astype(jnp.int32)).astype(jnp.float32).astype(jnp.bfloat16)
            for k in range(TOP)
        ]
        for chunk in range(model // width):
            cols = pl.ds(chunk * width, width)
            wide = answers[pl.ds(group * size, size), :, cols].astype(jnp.float32)
            rows_in = wide.reshape(slots, width).astype(jnp.bfloat16)
            parts = [
                jnp.dot(picks[k], rows_in, preferred_element_type=jnp.float32) * cols_v[:, TOP + k : TOP + k + 1]
                for k in range(TOP)
            ]
            finish(chunk, cols, parts[0] + parts[1])

    def begin(chunk, cols, part):
        total_v[:, cols] = tok_v[:, cols].astype(jnp.float32) + part

    def extend(chunk, cols, part):
        total_v[:, cols] = total_v[:, cols] + part

    puts = []

    def close(chunk, cols, part):
        tok_v[:, cols] = (total_v[:, cols] + part).astype(jnp.bfloat16)
        put = pltpu.make_async_copy(tok_v.at[:, cols], out.at[:, cols], local_sem.at[15 + chunk])
        put.start()
        puts.append(put)

    def combine(group, carry):
        answered(group, extend)
        return carry

    answered(0, begin)
    lax.fori_loop(1, GROUPS - 1, combine, 0)
    answered(GROUPS - 1, close)
    ref = mixed_v.at[pl.ds(0, positions - per)]
    pltpu.make_async_copy(ref, ref, swap_send.at[1]).wait()
    spatial.drained()
    scored.drained()
    valued.drained()
    temporal.drained()
    ref = outgoing.at[pl.ds(0, DEVICES - 1)]
    pltpu.make_async_copy(ref, ref, moe_send.at[0]).wait()
    pltpu.make_async_copy(ref, ref, moe_send.at[1]).wait()
    for put in puts:
        put.wait()


def number_slots(ids_v, gates_v, cols_v, slots_t, loads, clip, tm):
    for load in loads:
        load.wait()
    positions = ids_v.shape[1]
    expert = lax.broadcasted_iota(jnp.int32, (DEVICES, positions), 0)
    e_clip, e_tm = expert // TM, lax.rem(expert, TM)
    dz = lax.rem(e_clip // 2 - clip // 2 + 4, 4)
    dc = lax.rem(lax.rem(e_clip, 2) - lax.rem(clip, 2) + 2, 2)
    dy = lax.rem(e_tm // SIDE - tm // SIDE + 4, 4)
    dx = lax.rem(lax.rem(e_tm, SIDE) - lax.rem(tm, SIDE) + 4, 4)
    order = lax.rem((dz + 4 * dc + 8 * dy + 32 * dx) * INVERSE, DEVICES)
    named = [(ids_v[k : k + 1, :] == expert).astype(jnp.float32) for k in range(TOP)]
    rows = lax.broadcasted_iota(jnp.int32, (positions, positions), 0)
    cols = lax.broadcasted_iota(jnp.int32, (positions, positions), 1)
    before = (rows < cols).astype(jnp.float32).astype(jnp.bfloat16)
    counts = jnp.dot((named[0] + named[1]).astype(jnp.bfloat16), before, preferred_element_type=jnp.float32)
    row = (order * CAP).astype(jnp.float32) + counts
    table = jnp.zeros((DEVICES, positions), jnp.float32)
    for k in range(TOP):
        found = jnp.sum(named[k] * row, axis=0, keepdims=True)
        slots_t[k : k + 1, :] = found.astype(jnp.int32)
        table = jnp.where(expert == k, found, table)
        table = jnp.where(expert == TOP + k, gates_v[k : k + 1, :], table)
    cols_v[...] = table.T


def layer(tokens, sq, sk, sv, sproj, tqkv, tproj, mask, ids, gates, w_gate, w_up, w_down):
    positions, model = tokens.shape
    head_width = sq.shape[1]
    per = positions // TM
    hidden = w_gate.shape[1]
    bf16 = jnp.bfloat16
    vm = lambda *shape: pltpu.VMEM(shape, bf16)
    dma = lambda n: pltpu.SemaphoreType.DMA((n,))
    any_spec = pl.BlockSpec(memory_space=pl.ANY)
    return pl.pallas_call(
        layer_kernel,
        out_shape=jax.ShapeDtypeStruct((positions, model), bf16),
        in_specs=[any_spec] * 13,
        out_specs=any_spec,
        scratch_shapes=[
            vm(positions, model), vm(positions, head_width), vm(positions, model), vm(TM, per, model),
            vm(positions, 3 * head_width), vm(TM, per, head_width),
            pltpu.VMEM((positions, positions), jnp.float32), pltpu.VMEM((TM, TM), jnp.int32),
            pltpu.VMEM((TOP, positions), jnp.int32), pltpu.VMEM((TOP, positions), jnp.float32),
            vm(TM, sproj.shape[0], model), vm(TM, tqkv.shape[0], 3 * head_width), vm(TM, tproj.shape[0], model),
            vm(model, hidden), vm(model, hidden), vm(hidden, model),
            vm(DEVICES, CAP, model), vm(DEVICES, CAP, model), vm(DEVICES, CAP, model),
            vm(positions, hidden), pltpu.VMEM((positions, model), jnp.float32),
            pltpu.VMEM((positions, DEVICES), jnp.float32), pltpu.VMEM((8, positions), jnp.int32),
            vm(HEADS, positions, positions),
            dma(19), dma(4), dma(36), dma(36), dma(36), dma(36), dma(2), dma(2), dma(2), dma(GROUPS), dma(GROUPS),
        ],
        compiler_params=pltpu.CompilerParams(
            collective_id=0, has_side_effects=True, vmem_limit_bytes=67043328
        ),
        name="layer",
    )(tokens, sq, sk, sv, sproj, tqkv, tproj, mask, ids, gates, w_gate, w_up, w_down)


def shards(
    tokens,
    spatial_queries,
    spatial_keys,
    spatial_values,
    spatial_proj,
    temporal_qkv,
    temporal_proj,
    frame_mask,
    expert_ids,
    gate_values,
    expert_gate,
    expert_up,
    expert_down,
):
    positions, model_width = tokens.shape[2:]
    layer_out = layer(
        tokens.reshape(positions, model_width),
        spatial_queries.reshape(positions, -1),
        spatial_keys.reshape(positions, -1),
        spatial_values.reshape(positions, -1),
        spatial_proj,
        temporal_qkv,
        temporal_proj,
        frame_mask.reshape(frame_mask.shape[1:]),
        expert_ids.reshape(positions, TOP).T,
        gate_values.reshape(positions, TOP).T,
        expert_gate[0],
        expert_up[0],
        expert_down[0],
    )
    return layer_out.reshape(tokens.shape)


def solution(mesh):
    placed = (
        P("clip", "tm", None, None),
        P("clip", "tm", None, None),
        P("clip", "tm", None, None),
        P("clip", "tm", None, None),
        P("tm", None),
        P("tm", None),
        P("tm", None),
        P("clip", None, None),
        P("clip", "tm", None, None),
        P("clip", "tm", None, None),
        P(("clip", "tm"), None, None),
        P(("clip", "tm"), None, None),
        P(("clip", "tm"), None, None),
    )
    return jax.shard_map(
        shards, mesh=mesh, in_specs=placed, out_specs=P("clip", "tm", None, None), check_vma=False
    )
```

```python
import math

import jax
import jax.numpy as jnp
from jax import lax
from jax.experimental import pallas as pl
from jax.experimental.pallas import tpu as pltpu
from jax.sharding import PartitionSpec as P

HEADS = 8
HD = 128
TOP = 2
CAP = 8
SIDE = 4
TM = 16


EPS = 1e-06
MASKED = -1e30
MESH = pl.DeviceIdType.MESH
STRIDE = 49
INVERSE = pow(STRIDE, -1, 128)
GROUPS = 4
DEVICES = 128


class Gather:
    OFFSETS = (0, -1, 1, 2)
    EVENTS = ((-1, 0), (1, 0), (2, 0)) + tuple((i, j) for i in (0, -1, 1, 2) for j in (-1, 1)) + tuple(
        (i, 2) for i in (0, -1, 1, 2)
    )

    def __init__(self, shard, full, start, columns, place, send, recv, split):
        self.shard, self.full, self.send, self.recv = shard, full, send, recv
        self.start, self.columns, self.place, self.split = start, columns, place, split
        self.rows = full.shape[1]
        self.size = self.rows // 4 if split else self.rows // 2
        if split:
            self.base = place["parity"] * (self.rows // 2) + place["core"] * self.size
            self.other = (1 - place["parity"]) * (self.rows // 2) + place["core"] * self.size
        else:
            self.base = place["core"] * self.size

    def span(self, part):
        if part is None:
            return pl.ds(self.start, self.columns)
        return pl.ds(self.start + part * (self.columns // 2), self.columns // 2)

    def part(self, index, part=None, base=None):
        base = self.base if base is None else base
        return self.full.at[index, pl.ds(pl.multiple_of(base, self.size), self.size), self.span(part)]

    def own_part(self):
        return self.shard.at[pl.ds(pl.multiple_of(self.base, self.size), self.size), self.span(None)]

    def at(self, step1, step2):
        p = self.place
        return lax.rem(p["i1"] + step1 + SIDE, SIDE) * p["s1"] + lax.rem(p["i2"] + step2 + SIDE, SIDE) * p["s2"]

    def copy(self, src, dst, slot, clip, tm):
        pltpu.make_async_remote_copy(
            src_ref=src,
            dst_ref=dst,
            send_sem=self.send,
            recv_sem=self.recv.at[slot],
            device_id=(clip, tm),
            device_id_type=MESH,
        ).start()

    def arrived(self, ref, slot):
        pltpu.make_async_copy(ref, ref, self.recv.at[slot]).wait()

    def along(self, dim, way, src, dst, slot):
        target = self.at(way, 0) if dim == 1 else self.at(0, way)
        self.copy(src, dst, slot, self.place["clip"], target)

    def share(self, event):
        index = self.at(*self.EVENTS[event])
        whole = self.part(index)
        self.copy(whole, whole, 20, self.place["partner"], self.place["tm"])
        if self.split:
            for side in (0, 1):
                half = self.part(index, side)
                self.copy(half, half, 21 + event, self.place["above" if side == 0 else "below"], self.place["tm"])

    def lift(self, event):
        whole = self.part(self.at(*self.EVENTS[event]), base=self.other)
        self.arrived(whole, 21 + event)
        self.copy(whole, whole, 20, self.place["partner"], self.place["tm"])

    def second_dim(self, k):
        index = self.at(self.OFFSETS[k], 0)
        src = self.own_part() if k == 0 else self.part(index)
        self.along(2, 1, src, self.part(index), 4 + 2 * k)
        self.along(2, -1, src, self.part(index), 5 + 2 * k)
        if k > 0:
            self.share(k - 1)

    def own(self):
        mine = self.part(self.place["tm"])
        self.along(1, 1, self.own_part(), mine, 0)
        self.along(1, -1, self.own_part(), mine, 1)
        self.second_dim(0)

    def first_near(self):
        low, high = self.at(-1, 0), self.at(1, 0)
        self.arrived(self.part(low), 0)
        self.along(1, 1, self.part(low, 0), self.part(low, 0), 2)
        self.second_dim(1)
        self.arrived(self.part(high), 1)
        self.along(1, -1, self.part(high, 1), self.part(high, 1), 3)
        self.second_dim(2)

    def first_far(self):
        far = self.at(2, 0)
        self.arrived(self.part(far, 0), 2)
        self.arrived(self.part(far, 1), 3)
        self.second_dim(3)

    def second_near(self, k):
        step = self.OFFSETS[k]
        low, high = self.at(step, -1), self.at(step, 1)
        self.arrived(self.part(low), 4 + 2 * k)
        self.along(2, 1, self.part(low, 0), self.part(low, 0), 12 + 2 * k)
        self.share(3 + 2 * k)
        self.arrived(self.part(high), 5 + 2 * k)
        self.along(2, -1, self.part(high, 1), self.part(high, 1), 13 + 2 * k)
        self.share(4 + 2 * k)

    def second_far(self, k):
        far = self.at(self.OFFSETS[k], 2)
        self.arrived(self.part(far, 0), 12 + 2 * k)
        self.arrived(self.part(far, 1), 13 + 2 * k)
        self.share(11 + k)

    def pushed(self):
        self.arrived(self.full.at[pl.ds(0, TM - 1), pl.ds(0, self.rows // 2), self.span(None)], 20)

    def drained(self):
        ref = self.full.at[pl.ds(0, TM - 1), :, self.span(None)]
        pltpu.make_async_copy(ref, ref, self.send).wait()


def head_weights(queries, keys, head, bias):
    cols = pl.ds(pl.multiple_of(head * HD, HD), HD)
    scores = lax.dot_general(
        queries[:, cols], keys[:, cols], (((1,), (1,)), ((), ())), preferred_element_type=jnp.float32
    )
    scores = scores * (1.0 / math.sqrt(HD))
    if bias is not None:
        scores = jnp.where(bias[...] > 0.5, scores, MASKED)
    terms = jnp.exp(scores - jnp.max(scores, axis=-1, keepdims=True))
    return (terms * (1.0 / jnp.sum(terms, axis=-1, keepdims=True))).astype(jnp.bfloat16)


def head_mix(weights, values, out, head):
    cols = pl.ds(pl.multiple_of(head * HD, HD), HD)
    mixed = jnp.dot(weights, values[:, cols], preferred_element_type=jnp.float32)
    out[:, cols] = mixed.astype(jnp.bfloat16)


def layer_kernel(
    tokens, sq, sk, sv, sproj, tqkv, tproj, mask, ids, gates, w_gate, w_up, w_down,
    out,
    tok_v, mixed_v, normed_v, spread_v, qkv_v, home_v, allowed_v, mask_v, ids_v, gates_v,
    proj_s, qkv_w, proj_t, gate_w, up_w, down_w, outgoing, received, answers, hidden_v, total_v,
    cols_v, slots_t, inverse_v,
    local_sem, send_sem, recv_s, recv_q, recv_v, recv_t, swap_send, swap_recv, moe_send, go_recv, back_recv,
):
    clip = lax.axis_index("clip")
    tm = lax.axis_index("tm")
    core = lax.rem(clip, 2)
    y, x = tm // SIDE, lax.rem(tm, SIDE)
    positions = tok_v.shape[0]
    per = positions // TM
    head_width = HEADS * HD
    me = clip * TM + tm
    place = {
        "clip": clip,
        "tm": tm,
        "core": core,
        "partner": clip + 1 - 2 * core,
        "i1": x * (1 - core) + y * core,
        "i2": y * (1 - core) + x * core,
        "s1": 1 + 3 * core,
        "s2": 4 - 3 * core,
        "parity": lax.rem(clip // 2, 2),
        "above": lax.rem(clip + 2, DEVICES // TM),
        "below": lax.rem(clip + DEVICES // TM - 2, DEVICES // TM),
    }
    model = tok_v.shape[1]
    width = 512
    spatial = Gather(sproj, proj_s, 0, model, place, send_sem.at[0], recv_s, False)
    scored = Gather(tqkv, qkv_w, 0, 2 * head_width, place, send_sem.at[1], recv_q, True)
    valued = Gather(tqkv, qkv_w, 2 * head_width, head_width, place, send_sem.at[2], recv_v, True)
    temporal = Gather(tproj, proj_t, 0, model, place, send_sem.at[3], recv_t, True)

    loads = [
        pltpu.make_async_copy(src, dst, local_sem.at[n])
        for n, (src, dst) in enumerate(
            [
                (sq, qkv_v.at[:, pl.ds(0, head_width)]),
                (sk, qkv_v.at[:, pl.ds(head_width, head_width)]),
                (sv, qkv_v.at[:, pl.ds(2 * head_width, head_width)]),
                (tokens, tok_v),
                (sproj, proj_s.at[tm]), (tqkv, qkv_w.at[tm]), (tproj, proj_t.at[tm]), (mask, mask_v),
                (ids, ids_v), (gates, gates_v), (w_gate, gate_w), (w_up, up_w), (w_down, down_w),
            ]
        )
    ]
    for load in loads[:10]:
        load.start()

    barrier = pltpu.get_barrier_semaphore()

    clips = [lax.rem(clip + n, DEVICES // TM) for n in range(DEVICES // TM)]
    tms = [lax.rem(tm + n, TM) for n in range(TM)]
    for n in range(1, DEVICES):
        pl.semaphore_signal(
            barrier, inc=1, device_id=(clips[n // TM], tms[n % TM]), device_id_type=MESH
        )
    pl.semaphore_wait(barrier, DEVICES - 1)

    spatial.own()
    scored.own()

    for n in (0, 1, 2):
        loads[n].wait()
    triple_of = [qkv_v.at[:, pl.ds(n * head_width, head_width)] for n in range(3)]

    def mix_space(index, carry):
        for head in (2 * index, 2 * index + 1):
            head_mix(head_weights(triple_of[0], triple_of[1], head, None), triple_of[2], mixed_v, head)
        return carry

    lax.fori_loop(0, HEADS // 2, mix_space, 0)
    for load in loads[10:]:
        load.start()

    spatial.first_near()
    spatial.second_near(0)
    scored.first_near()
    scored.second_near(0)
    spatial.first_far()
    spatial.second_near(1)
    scored.first_far()
    scored.lift(0)
    spatial.second_near(2)
    scored.lift(1)
    spatial.second_far(0)
    scored.lift(3)
    scored.second_near(1)
    valued.own()
    scored.lift(4)
    scored.second_near(2)
    scored.second_far(0)
    scored.lift(2)
    valued.first_near()
    scored.lift(5)
    spatial.second_near(3)
    spatial.second_far(1)
    scored.lift(6)
    valued.first_far()
    scored.second_near(3)
    scored.lift(7)
    spatial.second_far(2)
    scored.second_far(1)
    scored.lift(8)
    valued.second_near(0)
    scored.second_far(2)
    valued.second_near(1)
    valued.second_near(2)
    spatial.second_far(3)
    valued.second_near(3)
    temporal.own()

    loads[3].wait()
    loads[4].wait()
    spatial.pushed()
    squares = jnp.zeros((positions, 1), jnp.float32)
    for chunk in range(model // width):
        cols = pl.ds(chunk * width, width)
        weights = proj_s[:, :, cols].reshape(head_width, width)
        update = jnp.dot(mixed_v[...], weights, preferred_element_type=jnp.float32)
        first = (tok_v[:, cols].astype(jnp.float32) + update).astype(jnp.bfloat16)
        tok_v[:, cols] = first
        wide = first.astype(jnp.float32)
        squares = squares + jnp.sum(wide * wide, axis=-1, keepdims=True)
    inverse_v[...] = lax.rsqrt(squares * (1.0 / model) + EPS)

    def block(index):
        return pl.ds(pl.multiple_of(index * per, per), per)

    def spread(shift, carry):
        other = lax.rem(tm + shift, TM)
        rows_at = block(other)
        normed_v[rows_at, :] = (tok_v[rows_at, :].astype(jnp.float32) * inverse_v[rows_at, :]).astype(jnp.bfloat16)

        @pl.when(shift < TM)
        def _():
            pltpu.make_async_remote_copy(
                src_ref=normed_v.at[rows_at],
                dst_ref=spread_v.at[tm],
                send_sem=swap_send.at[0],
                recv_sem=swap_recv.at[0],
                device_id=(clip, other),
                device_id_type=MESH,
            ).start()

        return carry

    lax.fori_loop(1, TM + 1, spread, 0)
    kept = pltpu.make_async_copy(normed_v.at[block(tm)], spread_v.at[tm], local_sem.at[13])
    kept.start()

    scored.second_far(3)
    valued.second_far(0)
    valued.second_far(1)
    valued.second_far(2)
    valued.second_far(3)
    scored.lift(11)
    scored.lift(9)
    scored.lift(10)
    scored.lift(12)
    valued.lift(0)
    valued.lift(1)
    valued.lift(2)

    rows = lax.broadcasted_iota(jnp.int32, (positions, TM), 0) // per
    cols16 = lax.broadcasted_iota(jnp.int32, (positions, TM), 1)
    frame_of = (rows == cols16).astype(jnp.float32)
    loads[7].wait()
    mask_f = jnp.where(mask_v[...] == 1, 1.0, 0.0)
    by_row = jnp.dot(frame_of, mask_f, preferred_element_type=jnp.float32)
    pairs = lax.dot_general(by_row, frame_of, (((1,), (1,)), ((), ())), preferred_element_type=jnp.float32)
    pos_r = lax.rem(lax.broadcasted_iota(jnp.int32, (positions, positions), 0), per)
    pos_c = lax.rem(lax.broadcasted_iota(jnp.int32, (positions, positions), 1), per)
    allowed_v[...] = jnp.where(pos_r == pos_c, pairs, 0.0)
    number_slots(ids_v, gates_v, cols_v, slots_t, loads[8:10], clip, tm)

    temporal.first_near()
    temporal.second_near(0)
    valued.lift(3)
    valued.lift(4)
    scored.lift(13)
    valued.lift(5)
    valued.lift(6)
    valued.lift(7)
    valued.lift(8)
    valued.lift(9)
    valued.lift(10)
    scored.lift(14)
    valued.lift(11)
    valued.lift(12)
    valued.lift(13)
    valued.lift(14)

    loads[5].wait()
    scored.pushed()
    ref = spread_v.at[pl.ds(0, TM - 1)]
    pltpu.make_async_copy(ref, ref, swap_recv.at[0]).wait()
    kept.wait()

    quarter = head_width // 4
    homes = []

    def triple(part, number):
        cols = pl.ds(part * head_width + number * quarter, quarter)
        weights = qkv_w[:, :, cols].reshape(model, quarter)
        rows_in = spread_v[...].reshape(positions, model)
        qkv_v[:, cols] = jnp.dot(rows_in, weights, preferred_element_type=jnp.float32).astype(jnp.bfloat16)

    def score_part(number):
        triple(0, number)
        triple(1, number)
        return [
            head_weights(triple_of[0], triple_of[1], head, allowed_v) for head in (2 * number, 2 * number + 1)
        ]

    def value_part(number, weights):
        triple(2, number)
        for n in range(2):
            head_mix(weights[n], triple_of[2], mixed_v, 2 * number + n)
        cols = pl.ds(number * quarter, quarter)

        def send(shift, carry):
            other = lax.rem(tm + shift, TM)
            pltpu.make_async_remote_copy(
                src_ref=mixed_v.at[block(other), cols],
                dst_ref=home_v.at[tm, :, cols],
                send_sem=swap_send.at[1],
                recv_sem=swap_recv.at[1 + number],
                device_id=(clip, other),
                device_id_type=MESH,
            ).start()
            return carry

        lax.fori_loop(1, TM, send, 0)
        home = pltpu.make_async_copy(mixed_v.at[block(tm), cols], home_v.at[tm, :, cols], local_sem.at[19 + number])
        home.start()
        homes.append(home)

    weights = score_part(0)

    valued.pushed()
    value_part(0, weights)

    temporal.first_far()
    temporal.second_near(1)

    weights = score_part(1)

    value_part(1, weights)

    temporal.second_near(2)

    weights = score_part(2)

    value_part(2, weights)

    temporal.second_far(0)
    temporal.second_far(1)
    temporal.second_near(3)

    weights = score_part(3)

    value_part(3, weights)

    temporal.second_far(2)
    temporal.second_far(3)
    temporal.lift(0)
    temporal.lift(1)
    temporal.lift(2)
    temporal.lift(3)
    temporal.lift(4)
    temporal.lift(5)
    temporal.lift(6)
    temporal.lift(7)
    temporal.lift(8)
    temporal.lift(9)
    temporal.lift(10)
    temporal.lift(11)
    temporal.lift(12)
    temporal.lift(13)
    temporal.lift(14)

    loads[6].wait()
    temporal.pushed()

    def come_home(number):
        ref = home_v.at[pl.ds(0, TM - 1), :, pl.ds(number * quarter, quarter)]
        pltpu.make_async_copy(ref, ref, swap_recv.at[1 + number]).wait()
        homes[number].wait()

    def back(half, cols):
        low = half * 2 * quarter
        weights = proj_t[half * (TM // 2) : (half + 1) * (TM // 2), :, cols].reshape(2 * quarter, width)
        rows_in = home_v[:, :, low : low + 2 * quarter].reshape(positions, 2 * quarter)
        return jnp.dot(rows_in, weights, preferred_element_type=jnp.float32)

    come_home(0)
    come_home(1)
    for chunk in range(model // width):
        cols = pl.ds(chunk * width, width)
        total_v[:, cols] = back(0, cols)
    come_home(2)
    come_home(3)
    squares = jnp.zeros((positions, 1), jnp.float32)
    for chunk in range(model // width):
        cols = pl.ds(chunk * width, width)
        update = (total_v[:, cols] + back(1, cols)).astype(jnp.bfloat16)
        second = (tok_v[:, cols].astype(jnp.float32) + update.astype(jnp.float32)).astype(jnp.bfloat16)
        tok_v[:, cols] = second
        wide = second.astype(jnp.float32)
        squares = squares + jnp.sum(wide * wide, axis=-1, keepdims=True)
    ref = normed_v.at[pl.ds(0, positions - per)]
    pltpu.make_async_copy(ref, ref, swap_send.at[0]).wait()
    inverse_v[...] = lax.rsqrt(squares * (1.0 / model) + EPS)

    def scale(index, carry):
        rows_at = pl.ds(pl.multiple_of(index * 32, 32), 32)
        normed_v[rows_at, :] = (tok_v[rows_at, :].astype(jnp.float32) * inverse_v[rows_at, :]).astype(jnp.bfloat16)
        return carry

    lax.fori_loop(0, positions // 32, scale, 0)


    size = DEVICES // GROUPS
    slots = size * CAP

    def ship(group, sign, src, dst, sends, receives):
        to_clip = [
            lax.rem(clip // 2 + sign * dz + 4, 4) * 2 + lax.rem(core + dc, 2) for dc in range(2) for dz in range(4)
        ]
        to_y = [lax.rem(y + sign * dy + 4, 4) * 4 for dy in range(4)]
        to_x = [lax.rem(x + sign * (dx + group) + 8, 4) for dx in range(4)]
        to_tm = [row + col for col in to_x for row in to_y]

        def send(message, offset):
            pltpu.make_async_remote_copy(
                src_ref=src.at[group * size + message],
                dst_ref=dst.at[group * size + message],
                send_sem=sends,
                recv_sem=receives.at[group],
                device_id=(to_clip[offset % 8], to_tm[offset // 8]),
                device_id_type=MESH,
            ).start()

        @pl.when(group > 0)
        def _():
            send(0, 0)

        for message in range(1, size):
            send(message, message * STRIDE % DEVICES)

    def landed(group, dst, receives):
        ref = dst.at[pl.ds(0, size)]
        pltpu.make_async_copy(ref, ref, receives.at[group]).wait()

    def pick(group, table):
        return (lax.broadcasted_iota(jnp.int32, (slots, positions), 0) + group * slots == table).astype(
            jnp.float32
        )

    def build(group, carry):
        chosen = pick(group, slots_t[0:1, :]) + pick(group, slots_t[1:2, :])
        chosen = chosen.astype(jnp.bfloat16)
        for chunk in range(model // width):
            cols = pl.ds(chunk * width, width)
            rows_out = jnp.dot(chosen, normed_v[:, cols], preferred_element_type=jnp.float32)
            outgoing[pl.ds(group * size, size), :, cols] = rows_out.reshape(size, CAP, width).astype(
                jnp.bfloat16
            )
        ship(group, 1, outgoing, received, moe_send.at[0], go_recv)
        return carry

    lax.fori_loop(0, GROUPS, build, 0)
    pltpu.make_async_copy(outgoing.at[0], received.at[0], go_recv.at[0]).start()
    for load in loads[10:]:
        load.wait()

    def serve(group, carry):
        landed(group, received, go_recv)
        mine = pl.ds(group * size, size)
        for chunk in range(model // width):
            cols = pl.ds(chunk * width, width)
            wide = received[mine, :, cols].astype(jnp.float32)
            normed_v[:, cols] = wide.reshape(slots, width).astype(jnp.bfloat16)

        def gate_up(cols):
            rows_in = normed_v[...]
            gate_part = jnp.dot(rows_in, gate_w[:, cols], preferred_element_type=jnp.float32)
            up_part = jnp.dot(rows_in, up_w[:, cols], preferred_element_type=jnp.float32)
            hidden_v[:, cols] = (gate_part / (1.0 + jnp.exp(-gate_part)) * up_part).astype(jnp.bfloat16)

        def gate_step(chunk, carry):
            gate_up(pl.ds(pl.multiple_of(chunk * 256, 256), 256))
            return carry

        hidden = hidden_v.shape[1]
        lax.fori_loop(0, hidden // 256, gate_step, 0)
        if hidden % 256:
            gate_up(pl.ds(hidden - hidden % 256, hidden % 256))

        def down_step(chunk, carry):
            cols = pl.ds(pl.multiple_of(chunk * width, width), width)
            answer = jnp.dot(hidden_v[...], down_w[:, cols], preferred_element_type=jnp.float32)
            received[mine, :, cols] = answer.reshape(size, CAP, width).astype(jnp.bfloat16)
            return carry

        lax.fori_loop(0, model // width, down_step, 0)
        ship(group, -1, received, answers, moe_send.at[1], back_recv)

        @pl.when(group == 0)
        def _():
            pltpu.make_async_copy(received.at[0], answers.at[0], back_recv.at[0]).start()

        return carry

    lax.fori_loop(0, GROUPS, serve, 0)

    def answered(group, finish):
        landed(group, answers, back_recv)
        lanes = lax.broadcasted_iota(jnp.int32, (positions, slots), 1) + group * slots
        picks = [
            (lanes == cols_v[:, k : k + 1].astype(jnp.int32)).astype(jnp.float32).astype(jnp.bfloat16)
            for k in range(TOP)
        ]
        for chunk in range(model // width):
            cols = pl.ds(chunk * width, width)
            wide = answers[pl.ds(group * size, size), :, cols].astype(jnp.float32)
            rows_in = wide.reshape(slots, width).astype(jnp.bfloat16)
            parts = [
                jnp.dot(picks[k], rows_in, preferred_element_type=jnp.float32) * cols_v[:, TOP + k : TOP + k + 1]
                for k in range(TOP)
            ]
            finish(chunk, cols, parts[0] + parts[1])

    def begin(chunk, cols, part):
        total_v[:, cols] = tok_v[:, cols].astype(jnp.float32) + part

    def extend(chunk, cols, part):
        total_v[:, cols] = total_v[:, cols] + part

    puts = []

    def close(chunk, cols, part):
        tok_v[:, cols] = (total_v[:, cols] + part).astype(jnp.bfloat16)
        put = pltpu.make_async_copy(tok_v.at[:, cols], out.at[:, cols], local_sem.at[15 + chunk])
        put.start()
        puts.append(put)

    def combine(group, carry):
        answered(group, extend)
        return carry

    answered(0, begin)
    lax.fori_loop(1, GROUPS - 1, combine, 0)
    answered(GROUPS - 1, close)
    ref = mixed_v.at[pl.ds(0, positions - per)]
    pltpu.make_async_copy(ref, ref, swap_send.at[1]).wait()
    spatial.drained()
    scored.drained()
    valued.drained()
    temporal.drained()
    ref = outgoing.at[pl.ds(0, DEVICES - 1)]
    pltpu.make_async_copy(ref, ref, moe_send.at[0]).wait()
    pltpu.make_async_copy(ref, ref, moe_send.at[1]).wait()
    for put in puts:
        put.wait()


def number_slots(ids_v, gates_v, cols_v, slots_t, loads, clip, tm):
    for load in loads:
        load.wait()
    positions = ids_v.shape[1]
    expert = lax.broadcasted_iota(jnp.int32, (DEVICES, positions), 0)
    e_clip, e_tm = expert // TM, lax.rem(expert, TM)
    dz = lax.rem(e_clip // 2 - clip // 2 + 4, 4)
    dc = lax.rem(lax.rem(e_clip, 2) - lax.rem(clip, 2) + 2, 2)
    dy = lax.rem(e_tm // SIDE - tm // SIDE + 4, 4)
    dx = lax.rem(lax.rem(e_tm, SIDE) - lax.rem(tm, SIDE) + 4, 4)
    order = lax.rem((dz + 4 * dc + 8 * dy + 32 * dx) * INVERSE, DEVICES)
    named = [(ids_v[k : k + 1, :] == expert).astype(jnp.float32) for k in range(TOP)]
    rows = lax.broadcasted_iota(jnp.int32, (positions, positions), 0)
    cols = lax.broadcasted_iota(jnp.int32, (positions, positions), 1)
    before = (rows < cols).astype(jnp.float32).astype(jnp.bfloat16)
    counts = jnp.dot((named[0] + named[1]).astype(jnp.bfloat16), before, preferred_element_type=jnp.float32)
    row = (order * CAP).astype(jnp.float32) + counts
    table = jnp.zeros((DEVICES, positions), jnp.float32)
    for k in range(TOP):
        found = jnp.sum(named[k] * row, axis=0, keepdims=True)
        slots_t[k : k + 1, :] = found.astype(jnp.int32)
        table = jnp.where(expert == k, found, table)
        table = jnp.where(expert == TOP + k, gates_v[k : k + 1, :], table)
    cols_v[...] = table.T


def layer(tokens, sq, sk, sv, sproj, tqkv, tproj, mask, ids, gates, w_gate, w_up, w_down):
    positions, model = tokens.shape
    head_width = sq.shape[1]
    per = positions // TM
    hidden = w_gate.shape[1]
    bf16 = jnp.bfloat16
    vm = lambda *shape: pltpu.VMEM(shape, bf16)
    dma = lambda n: pltpu.SemaphoreType.DMA((n,))
    any_spec = pl.BlockSpec(memory_space=pl.ANY)
    return pl.pallas_call(
        layer_kernel,
        out_shape=jax.ShapeDtypeStruct((positions, model), bf16),
        in_specs=[any_spec] * 13,
        out_specs=any_spec,
        scratch_shapes=[
            vm(positions, model), vm(positions, head_width), vm(positions, model), vm(TM, per, model),
            vm(positions, 3 * head_width), vm(TM, per, head_width),
            pltpu.VMEM((positions, positions), jnp.float32), pltpu.VMEM((TM, TM), jnp.int32),
            pltpu.VMEM((TOP, positions), jnp.int32), pltpu.VMEM((TOP, positions), jnp.float32),
            vm(TM, sproj.shape[0], model), vm(TM, tqkv.shape[0], 3 * head_width), vm(TM, tproj.shape[0], model),
            vm(model, hidden), vm(model, hidden), vm(hidden, model),
            vm(DEVICES, CAP, model), vm(DEVICES, CAP, model), vm(DEVICES, CAP, model),
            vm(positions, hidden), pltpu.VMEM((positions, model), jnp.float32),
            pltpu.VMEM((positions, DEVICES), jnp.float32), pltpu.VMEM((8, positions), jnp.int32),
            pltpu.VMEM((positions, 1), jnp.float32),
            dma(23), dma(4), dma(36), dma(36), dma(36), dma(36), dma(2), dma(5), dma(2), dma(GROUPS), dma(GROUPS),
        ],
        compiler_params=pltpu.CompilerParams(
            collective_id=0, has_side_effects=True, vmem_limit_bytes=67043328
        ),
        name="layer",
    )(tokens, sq, sk, sv, sproj, tqkv, tproj, mask, ids, gates, w_gate, w_up, w_down)


def shards(
    tokens,
    spatial_queries,
    spatial_keys,
    spatial_values,
    spatial_proj,
    temporal_qkv,
    temporal_proj,
    frame_mask,
    expert_ids,
    gate_values,
    expert_gate,
    expert_up,
    expert_down,
):
    positions, model_width = tokens.shape[2:]
    layer_out = layer(
        tokens.reshape(positions, model_width),
        spatial_queries.reshape(positions, -1),
        spatial_keys.reshape(positions, -1),
        spatial_values.reshape(positions, -1),
        spatial_proj,
        temporal_qkv,
        temporal_proj,
        frame_mask.reshape(frame_mask.shape[1:]),
        expert_ids.reshape(positions, TOP).T,
        gate_values.reshape(positions, TOP).T,
        expert_gate[0],
        expert_up[0],
        expert_down[0],
    )
    return layer_out.reshape(tokens.shape)


def solution(mesh):
    placed = (
        P("clip", "tm", None, None),
        P("clip", "tm", None, None),
        P("clip", "tm", None, None),
        P("clip", "tm", None, None),
        P("tm", None),
        P("tm", None),
        P("tm", None),
        P("clip", None, None),
        P("clip", "tm", None, None),
        P("clip", "tm", None, None),
        P(("clip", "tm"), None, None),
        P(("clip", "tm"), None, None),
        P(("clip", "tm"), None, None),
    )
    return jax.shard_map(
        shards, mesh=mesh, in_specs=placed, out_specs=P("clip", "tm", None, None), check_vma=False
    )
```

```python
import math

import jax
import jax.numpy as jnp
from jax import lax
from jax.experimental import pallas as pl
from jax.experimental.pallas import tpu as pltpu
from jax.sharding import PartitionSpec as P

HEADS = 8
HD = 128
TOP = 2
CAP = 8
SIDE = 4
TM = 16


EPS = 1e-06
MASKED = -1e30
MESH = pl.DeviceIdType.MESH
STRIDE = 49
INVERSE = pow(STRIDE, -1, 128)
GROUPS = 4
DEVICES = 128


class Gather:
    OFFSETS = (0, -1, 1, 2)
    EVENTS = ((-1, 0), (1, 0), (2, 0)) + tuple((i, j) for i in (0, -1, 1, 2) for j in (-1, 1)) + tuple(
        (i, 2) for i in (0, -1, 1, 2)
    )

    def __init__(self, full, start, columns, place, send, recv, split):
        self.full, self.send, self.recv = full, send, recv
        self.start, self.columns, self.place, self.split = start, columns, place, split
        self.rows = full.shape[1]
        self.size = self.rows // 4 if split else self.rows // 2
        if split:
            self.base = place["parity"] * (self.rows // 2) + place["core"] * self.size
            self.other = (1 - place["parity"]) * (self.rows // 2) + place["core"] * self.size
        else:
            self.base = place["core"] * self.size

    def span(self, part):
        if part is None:
            return pl.ds(self.start, self.columns)
        return pl.ds(self.start + part * (self.columns // 2), self.columns // 2)

    def part(self, index, part=None, base=None):
        base = self.base if base is None else base
        return self.full.at[index, pl.ds(pl.multiple_of(base, self.size), self.size), self.span(part)]

    def at(self, step1, step2):
        p = self.place
        return lax.rem(p["i1"] + step1 + SIDE, SIDE) * p["s1"] + lax.rem(p["i2"] + step2 + SIDE, SIDE) * p["s2"]

    def copy(self, src, dst, slot, clip, tm):
        pltpu.make_async_remote_copy(
            src_ref=src,
            dst_ref=dst,
            send_sem=self.send,
            recv_sem=self.recv.at[slot],
            device_id=(clip, tm),
            device_id_type=MESH,
        ).start()

    def arrived(self, ref, slot):
        pltpu.make_async_copy(ref, ref, self.recv.at[slot]).wait()

    def along(self, dim, way, src, dst, slot):
        target = self.at(way, 0) if dim == 1 else self.at(0, way)
        self.copy(src, dst, slot, self.place["clip"], target)

    def share(self, event):
        index = self.at(*self.EVENTS[event])
        whole = self.part(index)
        self.copy(whole, whole, 20, self.place["partner"], self.place["tm"])
        if self.split:
            for side in (0, 1):
                half = self.part(index, side)
                self.copy(half, half, 21 + event, self.place["above" if side == 0 else "below"], self.place["tm"])

    def lift(self, event):
        whole = self.part(self.at(*self.EVENTS[event]), base=self.other)
        self.arrived(whole, 21 + event)
        self.copy(whole, whole, 20, self.place["partner"], self.place["tm"])

    def second_dim(self, k):
        index = self.at(self.OFFSETS[k], 0)
        src = self.part(index)
        self.along(2, 1, src, self.part(index), 4 + 2 * k)
        self.along(2, -1, src, self.part(index), 5 + 2 * k)
        if k > 0:
            self.share(k - 1)

    def own(self):
        mine = self.part(self.place["tm"])
        self.along(1, 1, mine, mine, 0)
        self.along(1, -1, mine, mine, 1)
        self.second_dim(0)

    def first_near(self):
        low, high = self.at(-1, 0), self.at(1, 0)
        self.arrived(self.part(low), 0)
        self.along(1, 1, self.part(low, 0), self.part(low, 0), 2)
        self.second_dim(1)
        self.arrived(self.part(high), 1)
        self.along(1, -1, self.part(high, 1), self.part(high, 1), 3)
        self.second_dim(2)

    def first_far(self):
        far = self.at(2, 0)
        self.arrived(self.part(far, 0), 2)
        self.arrived(self.part(far, 1), 3)
        self.second_dim(3)

    def second_near(self, k):
        step = self.OFFSETS[k]
        low, high = self.at(step, -1), self.at(step, 1)
        self.arrived(self.part(low), 4 + 2 * k)
        self.along(2, 1, self.part(low, 0), self.part(low, 0), 12 + 2 * k)
        self.share(3 + 2 * k)
        self.arrived(self.part(high), 5 + 2 * k)
        self.along(2, -1, self.part(high, 1), self.part(high, 1), 13 + 2 * k)
        self.share(4 + 2 * k)

    def second_far(self, k):
        far = self.at(self.OFFSETS[k], 2)
        self.arrived(self.part(far, 0), 12 + 2 * k)
        self.arrived(self.part(far, 1), 13 + 2 * k)
        self.share(11 + k)

    def pushed(self):
        self.arrived(self.full.at[pl.ds(0, TM - 1), pl.ds(0, self.rows // 2), self.span(None)], 20)

    def drained(self):
        ref = self.full.at[pl.ds(0, TM - 1), :, self.span(None)]
        pltpu.make_async_copy(ref, ref, self.send).wait()


def head_weights(queries, keys, head, bias):
    cols = pl.ds(pl.multiple_of(head * HD, HD), HD)
    scores = lax.dot_general(
        queries[:, cols], keys[:, cols], (((1,), (1,)), ((), ())), preferred_element_type=jnp.float32
    )
    scores = scores * (math.log2(math.e) / math.sqrt(HD))
    if bias is not None:
        scores = scores + bias[...]
    terms = jnp.exp2(scores - jnp.max(scores, axis=-1, keepdims=True))
    return (terms * (1.0 / jnp.sum(terms, axis=-1, keepdims=True))).astype(jnp.bfloat16)


def head_mix(weights, values, out, head):
    cols = pl.ds(pl.multiple_of(head * HD, HD), HD)
    mixed = jnp.dot(weights, values[:, cols], preferred_element_type=jnp.float32)
    out[:, cols] = mixed.astype(jnp.bfloat16)


def layer_kernel(
    tokens, sq, sk, sv, sproj, tqkv, tproj, mask, ids, gates, w_gate, w_up, w_down,
    out,
    tok_v, mixed_v, normed_v, spread_v, qkv_v, home_v, allowed_v, mask_v, ids_v, gates_v,
    proj_s, qkv_w, proj_t, gate_w, up_w, down_w, outgoing, received, answers, hidden_v, total_v,
    cols_v, slots_t, inverse_v,
    local_sem, send_sem, recv_s, recv_q, recv_v, recv_t, swap_send, swap_recv, moe_send, go_recv, back_recv,
):
    clip = lax.axis_index("clip")
    tm = lax.axis_index("tm")
    core = lax.rem(clip, 2)
    y, x = tm // SIDE, lax.rem(tm, SIDE)
    positions = tok_v.shape[0]
    per = positions // TM
    head_width = HEADS * HD
    me = clip * TM + tm
    place = {
        "clip": clip,
        "tm": tm,
        "core": core,
        "partner": clip + 1 - 2 * core,
        "i1": x * (1 - core) + y * core,
        "i2": y * (1 - core) + x * core,
        "s1": 1 + 3 * core,
        "s2": 4 - 3 * core,
        "parity": lax.rem(clip // 2, 2),
        "above": lax.rem(clip + 2, DEVICES // TM),
        "below": lax.rem(clip + DEVICES // TM - 2, DEVICES // TM),
    }
    model = tok_v.shape[1]
    width = 512
    spatial = Gather(proj_s, 0, model, place, send_sem.at[0], recv_s, False)
    scored = Gather(qkv_w, 0, 2 * head_width, place, send_sem.at[1], recv_q, True)
    valued = Gather(qkv_w, 2 * head_width, head_width, place, send_sem.at[2], recv_v, True)
    temporal = Gather(proj_t, 0, model, place, send_sem.at[3], recv_t, True)

    loads = [
        pltpu.make_async_copy(src, dst, local_sem.at[n])
        for n, (src, dst) in enumerate(
            [
                (sq, qkv_v.at[:, pl.ds(0, head_width)]),
                (sk, qkv_v.at[:, pl.ds(head_width, head_width)]),
                (sv, qkv_v.at[:, pl.ds(2 * head_width, head_width)]),
                (tokens, tok_v),
                (sproj, proj_s.at[tm]), (tqkv, qkv_w.at[tm]), (tproj, proj_t.at[tm]), (mask, mask_v),
                (ids, ids_v), (gates, gates_v), (w_gate, gate_w), (w_up, up_w), (w_down, down_w),
            ]
        )
    ]
    for n in (4, 5, 0, 1, 2, 3, 6, 7, 8, 9):
        loads[n].start()

    barrier = pltpu.get_barrier_semaphore()

    clips = [lax.rem(clip + n, DEVICES // TM) for n in range(DEVICES // TM)]
    tms = [lax.rem(tm + n, TM) for n in range(TM)]
    for n in range(1, DEVICES):
        pl.semaphore_signal(
            barrier, inc=1, device_id=(clips[n // TM], tms[n % TM]), device_id_type=MESH
        )
    pl.semaphore_wait(barrier, DEVICES - 1)

    loads[4].wait()
    spatial.own()
    loads[5].wait()
    scored.own()

    for n in (0, 1, 2):
        loads[n].wait()
    triple_of = [qkv_v.at[:, pl.ds(n * head_width, head_width)] for n in range(3)]

    def mix_space(index, carry):
        for head in (2 * index, 2 * index + 1):
            head_mix(head_weights(triple_of[0], triple_of[1], head, None), triple_of[2], mixed_v, head)
        return carry

    lax.fori_loop(0, HEADS // 2, mix_space, 0)
    for load in loads[10:]:
        load.start()

    spatial.first_near()
    spatial.second_near(0)
    scored.second_near(0)
    spatial.first_far()
    scored.first_near()
    spatial.second_near(1)
    valued.own()
    spatial.second_near(2)
    scored.lift(3)
    spatial.second_far(0)
    scored.lift(4)
    scored.first_far()
    scored.second_far(0)
    scored.lift(0)
    valued.first_near()
    spatial.second_near(3)
    scored.lift(1)
    scored.lift(2)
    valued.first_far()
    scored.second_near(1)
    scored.lift(11)
    scored.second_near(2)
    valued.lift(0)
    spatial.second_far(1)
    valued.lift(1)
    valued.lift(2)
    spatial.second_far(2)
    scored.lift(5)
    scored.second_near(3)
    valued.second_near(0)
    valued.second_near(1)
    scored.lift(6)
    valued.second_near(2)
    spatial.second_far(3)
    scored.lift(7)
    valued.second_near(3)
    loads[6].wait()
    temporal.own()

    loads[3].wait()
    spatial.pushed()
    squares = jnp.zeros((positions, 1), jnp.float32)
    for chunk in range(model // width):
        cols = pl.ds(chunk * width, width)
        weights = proj_s[:, :, cols].reshape(head_width, width)
        update = jnp.dot(mixed_v[...], weights, preferred_element_type=jnp.float32)
        first = (tok_v[:, cols].astype(jnp.float32) + update).astype(jnp.bfloat16)
        tok_v[:, cols] = first
        wide = first.astype(jnp.float32)
        squares = squares + jnp.sum(wide * wide, axis=-1, keepdims=True)
    inverse_v[...] = lax.rsqrt(squares * (1.0 / model) + EPS)

    def block(index):
        return pl.ds(pl.multiple_of(index * per, per), per)

    def spread(shift, carry):
        other = lax.rem(tm + shift, TM)
        rows_at = block(other)
        normed_v[rows_at, :] = (tok_v[rows_at, :].astype(jnp.float32) * inverse_v[rows_at, :]).astype(jnp.bfloat16)

        @pl.when(shift < TM)
        def _():
            pltpu.make_async_remote_copy(
                src_ref=normed_v.at[rows_at],
                dst_ref=spread_v.at[tm],
                send_sem=swap_send.at[0],
                recv_sem=swap_recv.at[0],
                device_id=(clip, other),
                device_id_type=MESH,
            ).start()

        return carry

    lax.fori_loop(1, TM + 1, spread, 0)
    kept = pltpu.make_async_copy(normed_v.at[block(tm)], spread_v.at[tm], local_sem.at[13])
    kept.start()

    scored.lift(9)
    scored.second_far(1)
    valued.second_far(0)
    scored.lift(8)
    scored.second_far(2)

    rows = lax.broadcasted_iota(jnp.int32, (positions, TM), 0) // per
    cols16 = lax.broadcasted_iota(jnp.int32, (positions, TM), 1)
    frame_of = (rows == cols16).astype(jnp.float32)
    loads[7].wait()
    mask_f = jnp.where(mask_v[...] == 1, 1.0, 0.0)
    by_row = jnp.dot(frame_of, mask_f, preferred_element_type=jnp.float32)
    pairs = lax.dot_general(by_row, frame_of, (((1,), (1,)), ((), ())), preferred_element_type=jnp.float32)
    pos_r = lax.rem(lax.broadcasted_iota(jnp.int32, (positions, positions), 0), per)
    pos_c = lax.rem(lax.broadcasted_iota(jnp.int32, (positions, positions), 1), per)
    allowed_v[...] = jnp.where(jnp.where(pos_r == pos_c, pairs, 0.0) > 0.5, 0.0, MASKED)
    number_slots(ids_v, gates_v, cols_v, slots_t, loads[8:10], clip, tm)

    valued.second_far(3)
    valued.second_far(2)
    valued.lift(3)
    scored.second_far(3)
    scored.lift(10)
    valued.second_far(1)
    temporal.first_near()
    temporal.second_near(0)
    valued.lift(4)
    valued.lift(5)
    valued.lift(6)
    valued.lift(7)
    temporal.first_far()
    valued.lift(8)
    valued.lift(9)
    temporal.second_near(1)
    valued.lift(10)
    scored.lift(12)
    valued.lift(11)
    temporal.second_near(2)
    scored.lift(13)
    valued.lift(14)
    valued.lift(13)
    scored.lift(14)
    valued.lift(12)
    temporal.second_far(0)
    temporal.lift(0)
    temporal.lift(3)
    temporal.lift(1)
    temporal.lift(4)

    scored.pushed()
    ref = spread_v.at[pl.ds(0, TM - 1)]
    pltpu.make_async_copy(ref, ref, swap_recv.at[0]).wait()
    kept.wait()

    quarter = head_width // 4
    homes = []

    def triple(part, number):
        cols = pl.ds(part * head_width + number * quarter, quarter)
        weights = qkv_w[:, :, cols].reshape(model, quarter)
        rows_in = spread_v[...].reshape(positions, model)
        qkv_v[:, cols] = jnp.dot(rows_in, weights, preferred_element_type=jnp.float32).astype(jnp.bfloat16)

    def score_part(number):
        triple(0, number)
        triple(1, number)
        return [
            head_weights(triple_of[0], triple_of[1], head, allowed_v) for head in (2 * number, 2 * number + 1)
        ]

    def value_part(number, weights):
        triple(2, number)
        for n in range(2):
            head_mix(weights[n], triple_of[2], mixed_v, 2 * number + n)
        cols = pl.ds(number * quarter, quarter)

        def send(shift, carry):
            other = lax.rem(tm + shift, TM)
            pltpu.make_async_remote_copy(
                src_ref=mixed_v.at[block(other), cols],
                dst_ref=home_v.at[tm, :, cols],
                send_sem=swap_send.at[1],
                recv_sem=swap_recv.at[1 + number],
                device_id=(clip, other),
                device_id_type=MESH,
            ).start()
            return carry

        lax.fori_loop(1, TM, send, 0)
        home = pltpu.make_async_copy(mixed_v.at[block(tm), cols], home_v.at[tm, :, cols], local_sem.at[19 + number])
        home.start()
        homes.append(home)

    weights = score_part(0)
    temporal.second_near(3)
    valued.pushed()
    value_part(0, weights)
    temporal.lift(2)
    weights = score_part(1)
    temporal.second_far(1)
    value_part(1, weights)
    temporal.lift(6)
    temporal.lift(5)
    temporal.second_far(2)
    weights = score_part(2)
    temporal.lift(7)
    temporal.lift(11)
    value_part(2, weights)
    temporal.second_far(3)
    temporal.lift(8)
    weights = score_part(3)
    temporal.lift(12)
    value_part(3, weights)
    temporal.lift(9)
    temporal.lift(10)
    temporal.lift(13)
    temporal.lift(14)
    temporal.pushed()

    def come_home(number):
        ref = home_v.at[pl.ds(0, TM - 1), :, pl.ds(number * quarter, quarter)]
        pltpu.make_async_copy(ref, ref, swap_recv.at[1 + number]).wait()
        homes[number].wait()

    def back(half, cols):
        low = half * 2 * quarter
        weights = proj_t[half * (TM // 2) : (half + 1) * (TM // 2), :, cols].reshape(2 * quarter, width)
        rows_in = home_v[:, :, low : low + 2 * quarter].reshape(positions, 2 * quarter)
        return jnp.dot(rows_in, weights, preferred_element_type=jnp.float32)

    come_home(0)
    come_home(1)
    for chunk in range(model // width):
        cols = pl.ds(chunk * width, width)
        total_v[:, cols] = back(0, cols)
    come_home(2)
    come_home(3)
    squares = jnp.zeros((positions, 1), jnp.float32)
    for chunk in range(model // width):
        cols = pl.ds(chunk * width, width)
        update = (total_v[:, cols] + back(1, cols)).astype(jnp.bfloat16)
        second = (tok_v[:, cols].astype(jnp.float32) + update.astype(jnp.float32)).astype(jnp.bfloat16)
        tok_v[:, cols] = second
        wide = second.astype(jnp.float32)
        squares = squares + jnp.sum(wide * wide, axis=-1, keepdims=True)
    ref = normed_v.at[pl.ds(0, positions - per)]
    pltpu.make_async_copy(ref, ref, swap_send.at[0]).wait()
    inverse = lax.rsqrt(squares * (1.0 / model) + EPS)
    inverse_row = jnp.broadcast_to(inverse, (positions, 128)).T[0:1, :]

    size = DEVICES // GROUPS
    slots = size * CAP

    def ship(group, sign, src, dst, sends, receives):
        to_clip = [
            lax.rem(clip // 2 + sign * dz + 4, 4) * 2 + lax.rem(core + dc, 2) for dc in range(2) for dz in range(4)
        ]
        to_y = [lax.rem(y + sign * dy + 4, 4) * 4 for dy in range(4)]
        to_x = [lax.rem(x + sign * (dx + group) + 8, 4) for dx in range(4)]
        to_tm = [row + col for col in to_x for row in to_y]

        def send(message, offset):
            pltpu.make_async_remote_copy(
                src_ref=src.at[group * size + message],
                dst_ref=dst.at[group * size + message],
                send_sem=sends,
                recv_sem=receives.at[group + (group // (GROUPS - 1) if sign < 0 and message >= size // 2 else 0)],
                device_id=(to_clip[offset % 8], to_tm[offset // 8]),
                device_id_type=MESH,
            ).start()

        @pl.when(group > 0)
        def _():
            send(0, 0)

        for message in range(1, size):
            send(message, message * STRIDE % DEVICES)

    def landed(group, dst, receives, count=size):
        ref = dst.at[pl.ds(0, count)]
        pltpu.make_async_copy(ref, ref, receives.at[group]).wait()

    def pick(group, table):
        return (lax.broadcasted_iota(jnp.int32, (slots, positions), 0) + group * slots == table).astype(
            jnp.float32
        )

    def build(group, carry):
        chosen = pick(group, slots_t[0:1, :]) + pick(group, slots_t[1:2, :])
        factor = jnp.sum(chosen * inverse_row, axis=1, keepdims=True)
        chosen = chosen.astype(jnp.bfloat16)
        for chunk in range(model // width):
            cols = pl.ds(chunk * width, width)
            rows_out = jnp.dot(chosen, tok_v[:, cols], preferred_element_type=jnp.float32) * factor
            outgoing[pl.ds(group * size, size), :, cols] = rows_out.reshape(size, CAP, width).astype(
                jnp.bfloat16
            )
        ship(group, 1, outgoing, received, moe_send.at[0], go_recv)
        return carry

    lax.fori_loop(0, GROUPS, build, 0)
    pltpu.make_async_copy(outgoing.at[0], received.at[0], go_recv.at[0]).start()
    for load in loads[10:]:
        load.wait()

    def serve(group, carry):
        landed(group, received, go_recv)
        mine = pl.ds(group * size, size)
        for chunk in range(model // width):
            cols = pl.ds(chunk * width, width)
            wide = received[mine, :, cols].astype(jnp.float32)
            normed_v[:, cols] = wide.reshape(slots, width).astype(jnp.bfloat16)

        def gate_up(cols):
            rows_in = normed_v[...]
            gate_part = jnp.dot(rows_in, gate_w[:, cols], preferred_element_type=jnp.float32)
            up_part = jnp.dot(rows_in, up_w[:, cols], preferred_element_type=jnp.float32)
            hidden_v[:, cols] = (gate_part / (1.0 + jnp.exp(-gate_part)) * up_part).astype(jnp.bfloat16)

        def gate_step(chunk, carry):
            gate_up(pl.ds(pl.multiple_of(chunk * 256, 256), 256))
            return carry

        hidden = hidden_v.shape[1]
        lax.fori_loop(0, hidden // 256, gate_step, 0)
        if hidden % 256:
            gate_up(pl.ds(hidden - hidden % 256, hidden % 256))

        def down_step(chunk, carry):
            cols = pl.ds(pl.multiple_of(chunk * width, width), width)
            answer = jnp.dot(hidden_v[...], down_w[:, cols], preferred_element_type=jnp.float32)
            received[mine, :, cols] = answer.reshape(size, CAP, width).astype(jnp.bfloat16)
            return carry

        lax.fori_loop(0, model // width, down_step, 0)
        ship(group, -1, received, answers, moe_send.at[1], back_recv)

        @pl.when(group == 0)
        def _():
            pltpu.make_async_copy(received.at[0], answers.at[0], back_recv.at[0]).start()

        return carry

    lax.fori_loop(0, GROUPS, serve, 0)

    def answered(group, low, count, finish):
        landed(group, answers, back_recv, count)
        lanes = lax.broadcasted_iota(jnp.int32, (positions, count * CAP), 1) + low * CAP
        picks = [
            (lanes == cols_v[:, k : k + 1].astype(jnp.int32)).astype(jnp.float32).astype(jnp.bfloat16)
            for k in range(TOP)
        ]
        for chunk in range(model // width):
            cols = pl.ds(chunk * width, width)
            wide = answers[pl.ds(low, count), :, cols].astype(jnp.float32)
            rows_in = wide.reshape(count * CAP, width).astype(jnp.bfloat16)
            parts = [
                jnp.dot(picks[k], rows_in, preferred_element_type=jnp.float32) * cols_v[:, TOP + k : TOP + k + 1]
                for k in range(TOP)
            ]
            finish(chunk, cols, parts[0] + parts[1])

    def begin(chunk, cols, part):
        total_v[:, cols] = tok_v[:, cols].astype(jnp.float32) + part

    def extend(chunk, cols, part):
        total_v[:, cols] = total_v[:, cols] + part

    puts = []

    def close(chunk, cols, part):
        tok_v[:, cols] = (total_v[:, cols] + part).astype(jnp.bfloat16)
        put = pltpu.make_async_copy(tok_v.at[:, cols], out.at[:, cols], local_sem.at[15 + chunk])
        put.start()
        puts.append(put)

    def combine(group, carry):
        answered(group, group * size, size, extend)
        return carry

    answered(0, 0, size, begin)
    lax.fori_loop(1, GROUPS - 1, combine, 0)
    answered(GROUPS - 1, DEVICES - size, size // 2, extend)
    answered(GROUPS, DEVICES - size // 2, size // 2, close)
    ref = mixed_v.at[pl.ds(0, positions - per)]
    pltpu.make_async_copy(ref, ref, swap_send.at[1]).wait()
    spatial.drained()
    scored.drained()
    valued.drained()
    temporal.drained()
    ref = outgoing.at[pl.ds(0, DEVICES - 1)]
    pltpu.make_async_copy(ref, ref, moe_send.at[0]).wait()
    pltpu.make_async_copy(ref, ref, moe_send.at[1]).wait()
    for put in puts:
        put.wait()


def number_slots(ids_v, gates_v, cols_v, slots_t, loads, clip, tm):
    for load in loads:
        load.wait()
    positions = ids_v.shape[1]
    expert = lax.broadcasted_iota(jnp.int32, (DEVICES, positions), 0)
    e_clip, e_tm = expert // TM, lax.rem(expert, TM)
    dz = lax.rem(e_clip // 2 - clip // 2 + 4, 4)
    dc = lax.rem(lax.rem(e_clip, 2) - lax.rem(clip, 2) + 2, 2)
    dy = lax.rem(e_tm // SIDE - tm // SIDE + 4, 4)
    dx = lax.rem(lax.rem(e_tm, SIDE) - lax.rem(tm, SIDE) + 4, 4)
    order = lax.rem((dz + 4 * dc + 8 * dy + 32 * dx) * INVERSE, DEVICES)
    named = [(ids_v[k : k + 1, :] == expert).astype(jnp.float32) for k in range(TOP)]
    rows = lax.broadcasted_iota(jnp.int32, (positions, positions), 0)
    cols = lax.broadcasted_iota(jnp.int32, (positions, positions), 1)
    before = (rows < cols).astype(jnp.float32).astype(jnp.bfloat16)
    counts = jnp.dot((named[0] + named[1]).astype(jnp.bfloat16), before, preferred_element_type=jnp.float32)
    row = (order * CAP).astype(jnp.float32) + counts
    table = jnp.zeros((DEVICES, positions), jnp.float32)
    for k in range(TOP):
        found = jnp.sum(named[k] * row, axis=0, keepdims=True)
        slots_t[k : k + 1, :] = found.astype(jnp.int32)
        table = jnp.where(expert == k, found, table)
        table = jnp.where(expert == TOP + k, gates_v[k : k + 1, :], table)
    cols_v[...] = table.T


def layer(tokens, sq, sk, sv, sproj, tqkv, tproj, mask, ids, gates, w_gate, w_up, w_down):
    positions, model = tokens.shape
    head_width = sq.shape[1]
    per = positions // TM
    hidden = w_gate.shape[1]
    bf16 = jnp.bfloat16
    vm = lambda *shape: pltpu.VMEM(shape, bf16)
    dma = lambda n: pltpu.SemaphoreType.DMA((n,))
    any_spec = pl.BlockSpec(memory_space=pl.ANY)
    return pl.pallas_call(
        layer_kernel,
        out_shape=jax.ShapeDtypeStruct((positions, model), bf16),
        in_specs=[any_spec] * 13,
        out_specs=any_spec,
        scratch_shapes=[
            vm(positions, model), vm(positions, head_width), vm(positions, model), vm(TM, per, model),
            vm(positions, 3 * head_width), vm(TM, per, head_width),
            pltpu.VMEM((positions, positions), jnp.float32), pltpu.VMEM((TM, TM), jnp.int32),
            pltpu.VMEM((TOP, positions), jnp.int32), pltpu.VMEM((TOP, positions), jnp.float32),
            vm(TM, sproj.shape[0], model), vm(TM, tqkv.shape[0], 3 * head_width), vm(TM, tproj.shape[0], model),
            vm(model, hidden), vm(model, hidden), vm(hidden, model),
            vm(DEVICES, CAP, model), vm(DEVICES, CAP, model), vm(DEVICES, CAP, model),
            vm(positions, hidden), pltpu.VMEM((positions, model), jnp.float32),
            pltpu.VMEM((positions, DEVICES), jnp.float32), pltpu.VMEM((8, positions), jnp.int32),
            pltpu.VMEM((positions, 1), jnp.float32),
            dma(23), dma(4), dma(36), dma(36), dma(36), dma(36), dma(2), dma(5), dma(2), dma(GROUPS), dma(GROUPS + 1),
        ],
        compiler_params=pltpu.CompilerParams(
            collective_id=0, has_side_effects=True, vmem_limit_bytes=67043328
        ),
        name="layer",
    )(tokens, sq, sk, sv, sproj, tqkv, tproj, mask, ids, gates, w_gate, w_up, w_down)


def shards(
    tokens,
    spatial_queries,
    spatial_keys,
    spatial_values,
    spatial_proj,
    temporal_qkv,
    temporal_proj,
    frame_mask,
    expert_ids,
    gate_values,
    expert_gate,
    expert_up,
    expert_down,
):
    positions, model_width = tokens.shape[2:]
    layer_out = layer(
        tokens.reshape(positions, model_width),
        spatial_queries.reshape(positions, -1),
        spatial_keys.reshape(positions, -1),
        spatial_values.reshape(positions, -1),
        spatial_proj,
        temporal_qkv,
        temporal_proj,
        frame_mask.reshape(frame_mask.shape[1:]),
        expert_ids.reshape(positions, TOP).T,
        gate_values.reshape(positions, TOP).T,
        expert_gate[0],
        expert_up[0],
        expert_down[0],
    )
    return layer_out.reshape(tokens.shape)


def solution(mesh):
    placed = (
        P("clip", "tm", None, None),
        P("clip", "tm", None, None),
        P("clip", "tm", None, None),
        P("clip", "tm", None, None),
        P("tm", None),
        P("tm", None),
        P("tm", None),
        P("clip", None, None),
        P("clip", "tm", None, None),
        P("clip", "tm", None, None),
        P(("clip", "tm"), None, None),
        P(("clip", "tm"), None, None),
        P(("clip", "tm"), None, None),
    )
    return jax.shard_map(
        shards, mesh=mesh, in_specs=placed, out_specs=P("clip", "tm", None, None), check_vma=False
    )
```

```python
import math

import jax
import jax.numpy as jnp
from jax import lax
from jax.experimental import pallas as pl
from jax.experimental.pallas import tpu as pltpu
from jax.sharding import PartitionSpec as P

HEADS = 8
HD = 128
TOP = 2
CAP = 8
SIDE = 4
TM = 16


EPS = 1e-06
MASKED = -1e30
MESH = pl.DeviceIdType.MESH
STRIDE = 49
INVERSE = pow(STRIDE, -1, 128)
GROUPS = 4
DEVICES = 128


class Gather:
    OFFSETS = (0, -1, 1, 2)
    EVENTS = ((-1, 0), (1, 0), (2, 0)) + tuple((i, j) for i in (0, -1, 1, 2) for j in (-1, 1)) + tuple(
        (i, 2) for i in (0, -1, 1, 2)
    )

    def __init__(self, full, start, columns, place, send, recv, split):
        self.full, self.send, self.recv = full, send, recv
        self.start, self.columns, self.place, self.split = start, columns, place, split
        self.rows = full.shape[1]
        self.size = self.rows // 4 if split else self.rows // 2
        if split:
            self.base = place["parity"] * (self.rows // 2) + place["core"] * self.size
            self.other = (1 - place["parity"]) * (self.rows // 2) + place["core"] * self.size
        else:
            self.base = place["core"] * self.size

    def span(self, part):
        if part is None:
            return pl.ds(self.start, self.columns)
        return pl.ds(self.start + part * (self.columns // 2), self.columns // 2)

    def part(self, index, part=None, base=None):
        base = self.base if base is None else base
        return self.full.at[index, pl.ds(pl.multiple_of(base, self.size), self.size), self.span(part)]

    def at(self, step1, step2):
        p = self.place
        return lax.rem(p["i1"] + step1 + SIDE, SIDE) * p["s1"] + lax.rem(p["i2"] + step2 + SIDE, SIDE) * p["s2"]

    def copy(self, src, dst, slot, clip, tm):
        pltpu.make_async_remote_copy(
            src_ref=src,
            dst_ref=dst,
            send_sem=self.send,
            recv_sem=self.recv.at[slot],
            device_id=(clip, tm),
            device_id_type=MESH,
        ).start()

    def arrived(self, ref, slot):
        pltpu.make_async_copy(ref, ref, self.recv.at[slot]).wait()

    def along(self, dim, way, src, dst, slot):
        target = self.at(way, 0) if dim == 1 else self.at(0, way)
        self.copy(src, dst, slot, self.place["clip"], target)

    def share(self, event):
        index = self.at(*self.EVENTS[event])
        whole = self.part(index)
        self.copy(whole, whole, 20, self.place["partner"], self.place["tm"])
        if self.split:
            for side in (0, 1):
                half = self.part(index, side)
                self.copy(half, half, 21 + event, self.place["above" if side == 0 else "below"], self.place["tm"])

    def lift(self, event):
        whole = self.part(self.at(*self.EVENTS[event]), base=self.other)
        self.arrived(whole, 21 + event)
        self.copy(whole, whole, 20, self.place["partner"], self.place["tm"])

    def second_dim(self, k):
        index = self.at(self.OFFSETS[k], 0)
        src = self.part(index)
        self.along(2, 1, src, self.part(index), 4 + 2 * k)
        self.along(2, -1, src, self.part(index), 5 + 2 * k)
        if k > 0:
            self.share(k - 1)

    def own(self):
        mine = self.part(self.place["tm"])
        self.along(1, 1, mine, mine, 0)
        self.along(1, -1, mine, mine, 1)
        self.second_dim(0)

    def first_near(self):
        low, high = self.at(-1, 0), self.at(1, 0)
        self.arrived(self.part(low), 0)
        self.along(1, 1, self.part(low, 0), self.part(low, 0), 2)
        self.second_dim(1)
        self.arrived(self.part(high), 1)
        self.along(1, -1, self.part(high, 1), self.part(high, 1), 3)
        self.second_dim(2)

    def first_far(self):
        far = self.at(2, 0)
        self.arrived(self.part(far, 0), 2)
        self.arrived(self.part(far, 1), 3)
        self.second_dim(3)

    def second_near(self, k):
        step = self.OFFSETS[k]
        low, high = self.at(step, -1), self.at(step, 1)
        self.arrived(self.part(low), 4 + 2 * k)
        self.along(2, 1, self.part(low, 0), self.part(low, 0), 12 + 2 * k)
        self.share(3 + 2 * k)
        self.arrived(self.part(high), 5 + 2 * k)
        self.along(2, -1, self.part(high, 1), self.part(high, 1), 13 + 2 * k)
        self.share(4 + 2 * k)

    def second_far(self, k):
        far = self.at(self.OFFSETS[k], 2)
        self.arrived(self.part(far, 0), 12 + 2 * k)
        self.arrived(self.part(far, 1), 13 + 2 * k)
        self.share(11 + k)

    def pushed(self):
        self.arrived(self.full.at[pl.ds(0, TM - 1), pl.ds(0, self.rows // 2), self.span(None)], 20)

    def drained(self):
        ref = self.full.at[pl.ds(0, TM - 1), :, self.span(None)]
        pltpu.make_async_copy(ref, ref, self.send).wait()


def head_weights(queries, keys, head, bias):
    cols = pl.ds(pl.multiple_of(head * HD, HD), HD)
    scores = lax.dot_general(
        queries[:, cols], keys[:, cols], (((1,), (1,)), ((), ())), preferred_element_type=jnp.float32
    )
    scores = scores * (math.log2(math.e) / math.sqrt(HD))
    if bias is not None:
        scores = scores + bias[...]
    terms = jnp.exp2(scores - jnp.max(scores, axis=-1, keepdims=True))
    return (terms * (1.0 / jnp.sum(terms, axis=-1, keepdims=True))).astype(jnp.bfloat16)


def head_mix(weights, values, out, head):
    cols = pl.ds(pl.multiple_of(head * HD, HD), HD)
    mixed = jnp.dot(weights, values[:, cols], preferred_element_type=jnp.float32)
    out[:, cols] = mixed.astype(jnp.bfloat16)


def layer_kernel(
    tokens, sq, sk, sv, sproj, tqkv, tproj, mask, ids, gates, w_gate, w_up, w_down,
    out,
    tok_v, mixed_v, normed_v, spread_v, qkv_v, home_v, allowed_v, mask_v, ids_v, gates_v,
    proj_s, qkv_w, proj_t, gate_w, up_w, down_w, outgoing, received, answers, hidden_v, total_v,
    cols_v, slots_t, inverse_v,
    local_sem, send_sem, recv_s, recv_q, recv_v, recv_t, swap_send, swap_recv, moe_send, go_recv, back_recv,
):
    clip = lax.axis_index("clip")
    tm = lax.axis_index("tm")
    core = lax.rem(clip, 2)
    y, x = tm // SIDE, lax.rem(tm, SIDE)
    positions = tok_v.shape[0]
    per = positions // TM
    head_width = HEADS * HD
    me = clip * TM + tm
    place = {
        "clip": clip,
        "tm": tm,
        "core": core,
        "partner": clip + 1 - 2 * core,
        "i1": x * (1 - core) + y * core,
        "i2": y * (1 - core) + x * core,
        "s1": 1 + 3 * core,
        "s2": 4 - 3 * core,
        "parity": lax.rem(clip // 2, 2),
        "above": lax.rem(clip + 2, DEVICES // TM),
        "below": lax.rem(clip + DEVICES // TM - 2, DEVICES // TM),
    }
    model = tok_v.shape[1]
    width = 512
    spatial = Gather(proj_s, 0, model, place, send_sem.at[0], recv_s, False)
    scored = Gather(qkv_w, 0, 2 * head_width, place, send_sem.at[1], recv_q, True)
    valued = Gather(qkv_w, 2 * head_width, head_width, place, send_sem.at[2], recv_v, True)
    temporal = Gather(proj_t, 0, model, place, send_sem.at[3], recv_t, True)

    loads = [
        pltpu.make_async_copy(src, dst, local_sem.at[n])
        for n, (src, dst) in enumerate(
            [
                (sq, qkv_v.at[:, pl.ds(0, head_width)]),
                (sk, qkv_v.at[:, pl.ds(head_width, head_width)]),
                (sv, qkv_v.at[:, pl.ds(2 * head_width, head_width)]),
                (tokens, tok_v),
                (sproj, proj_s.at[tm]), (tqkv, qkv_w.at[tm]), (tproj, proj_t.at[tm]), (mask, mask_v),
                (ids, ids_v), (gates, gates_v), (w_gate, gate_w), (w_up, up_w), (w_down, down_w),
            ]
        )
    ]
    for n in (4, 5, 0, 1, 2, 3, 6, 7, 8, 9):
        loads[n].start()

    barrier = pltpu.get_barrier_semaphore()

    clips = [lax.rem(clip + n, DEVICES // TM) for n in range(DEVICES // TM)]
    tms = [lax.rem(tm + n, TM) for n in range(TM)]
    for n in range(1, DEVICES):
        pl.semaphore_signal(
            barrier, inc=1, device_id=(clips[n // TM], tms[n % TM]), device_id_type=MESH
        )
    pl.semaphore_wait(barrier, DEVICES - 1)

    loads[4].wait()
    spatial.own()
    loads[5].wait()
    scored.own()

    for n in (0, 1, 2):
        loads[n].wait()
    triple_of = [qkv_v.at[:, pl.ds(n * head_width, head_width)] for n in range(3)]

    def mix_space(index, carry):
        for head in (2 * index, 2 * index + 1):
            head_mix(head_weights(triple_of[0], triple_of[1], head, None), triple_of[2], mixed_v, head)
        return carry

    lax.fori_loop(0, HEADS // 2, mix_space, 0)
    for load in loads[10:]:
        load.start()

    spatial.first_near()
    spatial.second_near(0)
    scored.first_near()
    scored.second_near(0)
    spatial.first_far()
    spatial.second_near(1)
    scored.first_far()
    scored.lift(0)
    spatial.second_near(2)
    scored.lift(1)
    spatial.second_far(0)
    scored.lift(3)
    scored.second_near(1)
    valued.own()
    scored.lift(4)
    scored.second_near(2)
    scored.second_far(0)
    scored.lift(2)
    valued.first_near()
    scored.lift(5)
    spatial.second_near(3)
    spatial.second_far(1)
    scored.lift(6)
    valued.first_far()
    scored.second_near(3)
    scored.lift(7)
    spatial.second_far(2)
    scored.second_far(1)
    scored.lift(8)
    valued.second_near(0)
    scored.second_far(2)
    valued.second_near(1)
    valued.second_near(2)
    spatial.second_far(3)
    valued.second_near(3)
    loads[6].wait()
    temporal.own()

    loads[3].wait()
    spatial.pushed()
    squares = jnp.zeros((positions, 1), jnp.float32)
    for chunk in range(model // width):
        cols = pl.ds(chunk * width, width)
        weights = proj_s[:, :, cols].reshape(head_width, width)
        update = jnp.dot(mixed_v[...], weights, preferred_element_type=jnp.float32)
        first = (tok_v[:, cols].astype(jnp.float32) + update).astype(jnp.bfloat16)
        tok_v[:, cols] = first
        wide = first.astype(jnp.float32)
        squares = squares + jnp.sum(wide * wide, axis=-1, keepdims=True)
    inverse_v[...] = lax.rsqrt(squares * (1.0 / model) + EPS)

    def block(index):
        return pl.ds(pl.multiple_of(index * per, per), per)

    def spread(shift, carry):
        other = lax.rem(tm + shift, TM)
        rows_at = block(other)
        normed_v[rows_at, :] = (tok_v[rows_at, :].astype(jnp.float32) * inverse_v[rows_at, :]).astype(jnp.bfloat16)

        @pl.when(shift < TM)
        def _():
            pltpu.make_async_remote_copy(
                src_ref=normed_v.at[rows_at],
                dst_ref=spread_v.at[tm],
                send_sem=swap_send.at[0],
                recv_sem=swap_recv.at[0],
                device_id=(clip, other),
                device_id_type=MESH,
            ).start()

        return carry

    lax.fori_loop(1, TM + 1, spread, 0)
    kept = pltpu.make_async_copy(normed_v.at[block(tm)], spread_v.at[tm], local_sem.at[13])
    kept.start()

    scored.second_far(3)
    valued.second_far(0)
    valued.second_far(1)
    valued.second_far(2)
    valued.second_far(3)
    scored.lift(11)
    scored.lift(9)
    scored.lift(10)
    scored.lift(12)
    valued.lift(0)
    valued.lift(1)
    valued.lift(2)

    rows = lax.broadcasted_iota(jnp.int32, (positions, TM), 0) // per
    cols16 = lax.broadcasted_iota(jnp.int32, (positions, TM), 1)
    frame_of = (rows == cols16).astype(jnp.float32)
    loads[7].wait()
    mask_f = jnp.where(mask_v[...] == 1, 1.0, 0.0)
    by_row = jnp.dot(frame_of, mask_f, preferred_element_type=jnp.float32)
    pairs = lax.dot_general(by_row, frame_of, (((1,), (1,)), ((), ())), preferred_element_type=jnp.float32)
    pos_r = lax.rem(lax.broadcasted_iota(jnp.int32, (positions, positions), 0), per)
    pos_c = lax.rem(lax.broadcasted_iota(jnp.int32, (positions, positions), 1), per)
    allowed_v[...] = jnp.where(jnp.where(pos_r == pos_c, pairs, 0.0) > 0.5, 0.0, MASKED)
    number_slots(ids_v, gates_v, cols_v, slots_t, loads[8:10], clip, tm)

    temporal.first_near()
    temporal.second_near(0)
    valued.lift(3)
    valued.lift(4)
    scored.lift(13)
    valued.lift(5)
    valued.lift(6)
    valued.lift(7)
    temporal.first_far()
    valued.lift(8)
    valued.lift(9)
    temporal.second_near(1)
    valued.lift(10)
    scored.lift(14)
    valued.lift(11)
    temporal.second_near(2)
    valued.lift(12)
    valued.lift(13)
    valued.lift(14)
    temporal.second_far(0)
    temporal.lift(0)
    temporal.lift(1)
    temporal.lift(3)
    temporal.lift(4)

    scored.pushed()
    ref = spread_v.at[pl.ds(0, TM - 1)]
    pltpu.make_async_copy(ref, ref, swap_recv.at[0]).wait()
    kept.wait()

    quarter = head_width // 4
    homes = []

    def triple(part, number):
        cols = pl.ds(part * head_width + number * quarter, quarter)
        weights = qkv_w[:, :, cols].reshape(model, quarter)
        rows_in = spread_v[...].reshape(positions, model)
        qkv_v[:, cols] = jnp.dot(rows_in, weights, preferred_element_type=jnp.float32).astype(jnp.bfloat16)

    def score_part(number):
        triple(0, number)
        triple(1, number)
        return [
            head_weights(triple_of[0], triple_of[1], head, allowed_v) for head in (2 * number, 2 * number + 1)
        ]

    def value_part(number, weights):
        triple(2, number)
        for n in range(2):
            head_mix(weights[n], triple_of[2], mixed_v, 2 * number + n)
        cols = pl.ds(number * quarter, quarter)

        def send(shift, carry):
            other = lax.rem(tm + shift, TM)
            pltpu.make_async_remote_copy(
                src_ref=mixed_v.at[block(other), cols],
                dst_ref=home_v.at[tm, :, cols],
                send_sem=swap_send.at[1],
                recv_sem=swap_recv.at[1 + number],
                device_id=(clip, other),
                device_id_type=MESH,
            ).start()
            return carry

        lax.fori_loop(1, TM, send, 0)
        home = pltpu.make_async_copy(mixed_v.at[block(tm), cols], home_v.at[tm, :, cols], local_sem.at[19 + number])
        home.start()
        homes.append(home)

    weights = score_part(0)
    temporal.second_near(3)
    valued.pushed()
    value_part(0, weights)
    temporal.lift(2)
    weights = score_part(1)
    temporal.second_far(1)
    value_part(1, weights)
    temporal.lift(6)
    temporal.lift(5)
    temporal.second_far(2)
    weights = score_part(2)
    temporal.lift(7)
    temporal.lift(11)
    value_part(2, weights)
    temporal.second_far(3)
    temporal.lift(8)
    weights = score_part(3)
    temporal.lift(12)
    value_part(3, weights)
    temporal.lift(9)
    temporal.lift(10)
    temporal.lift(13)
    temporal.lift(14)
    temporal.pushed()

    def come_home(number):
        ref = home_v.at[pl.ds(0, TM - 1), :, pl.ds(number * quarter, quarter)]
        pltpu.make_async_copy(ref, ref, swap_recv.at[1 + number]).wait()
        homes[number].wait()

    def back(half, cols):
        low = half * 2 * quarter
        weights = proj_t[half * (TM // 2) : (half + 1) * (TM // 2), :, cols].reshape(2 * quarter, width)
        rows_in = home_v[:, :, low : low + 2 * quarter].reshape(positions, 2 * quarter)
        return jnp.dot(rows_in, weights, preferred_element_type=jnp.float32)

    come_home(0)
    come_home(1)
    for chunk in range(model // width):
        cols = pl.ds(chunk * width, width)
        total_v[:, cols] = back(0, cols)
    come_home(2)
    come_home(3)
    squares = jnp.zeros((positions, 1), jnp.float32)
    for chunk in range(model // width):
        cols = pl.ds(chunk * width, width)
        update = (total_v[:, cols] + back(1, cols)).astype(jnp.bfloat16)
        second = (tok_v[:, cols].astype(jnp.float32) + update.astype(jnp.float32)).astype(jnp.bfloat16)
        tok_v[:, cols] = second
        wide = second.astype(jnp.float32)
        squares = squares + jnp.sum(wide * wide, axis=-1, keepdims=True)
    ref = normed_v.at[pl.ds(0, positions - per)]
    pltpu.make_async_copy(ref, ref, swap_send.at[0]).wait()
    inverse = lax.rsqrt(squares * (1.0 / model) + EPS)
    inverse_row = jnp.broadcast_to(inverse, (positions, 128)).T[0:1, :]

    size = DEVICES // GROUPS
    slots = size * CAP

    def ship(group, sign, src, dst, sends, receives):
        to_clip = [
            lax.rem(clip // 2 + sign * dz + 4, 4) * 2 + lax.rem(core + dc, 2) for dc in range(2) for dz in range(4)
        ]
        to_y = [lax.rem(y + sign * dy + 4, 4) * 4 for dy in range(4)]
        to_x = [lax.rem(x + sign * (dx + group) + 8, 4) for dx in range(4)]
        to_tm = [row + col for col in to_x for row in to_y]

        def send(message, offset):
            pltpu.make_async_remote_copy(
                src_ref=src.at[group * size + message],
                dst_ref=dst.at[group * size + message],
                send_sem=sends,
                recv_sem=receives.at[group + (group // (GROUPS - 1) if sign < 0 and message >= size // 2 else 0)],
                device_id=(to_clip[offset % 8], to_tm[offset // 8]),
                device_id_type=MESH,
            ).start()

        @pl.when(group > 0)
        def _():
            send(0, 0)

        for message in range(1, size):
            send(message, message * STRIDE % DEVICES)

    def landed(group, dst, receives, count=size):
        ref = dst.at[pl.ds(0, count)]
        pltpu.make_async_copy(ref, ref, receives.at[group]).wait()

    def pick(group, table):
        return (lax.broadcasted_iota(jnp.int32, (slots, positions), 0) + group * slots == table).astype(
            jnp.float32
        )

    def build(group, carry):
        chosen = pick(group, slots_t[0:1, :]) + pick(group, slots_t[1:2, :])
        factor = jnp.sum(chosen * inverse_row, axis=1, keepdims=True)
        chosen = chosen.astype(jnp.bfloat16)
        for chunk in range(model // width):
            cols = pl.ds(chunk * width, width)
            rows_out = jnp.dot(chosen, tok_v[:, cols], preferred_element_type=jnp.float32) * factor
            outgoing[pl.ds(group * size, size), :, cols] = rows_out.reshape(size, CAP, width).astype(
                jnp.bfloat16
            )
        ship(group, 1, outgoing, received, moe_send.at[0], go_recv)
        return carry

    lax.fori_loop(0, GROUPS, build, 0)
    pltpu.make_async_copy(outgoing.at[0], received.at[0], go_recv.at[0]).start()
    for load in loads[10:]:
        load.wait()

    def serve(group, carry):
        landed(group, received, go_recv)
        mine = pl.ds(group * size, size)
        for chunk in range(model // width):
            cols = pl.ds(chunk * width, width)
            wide = received[mine, :, cols].astype(jnp.float32)
            normed_v[:, cols] = wide.reshape(slots, width).astype(jnp.bfloat16)

        def gate_up(cols):
            rows_in = normed_v[...]
            gate_part = jnp.dot(rows_in, gate_w[:, cols], preferred_element_type=jnp.float32)
            up_part = jnp.dot(rows_in, up_w[:, cols], preferred_element_type=jnp.float32)
            hidden_v[:, cols] = (gate_part / (1.0 + jnp.exp(-gate_part)) * up_part).astype(jnp.bfloat16)

        def gate_step(chunk, carry):
            gate_up(pl.ds(pl.multiple_of(chunk * 256, 256), 256))
            return carry

        hidden = hidden_v.shape[1]
        lax.fori_loop(0, hidden // 256, gate_step, 0)
        if hidden % 256:
            gate_up(pl.ds(hidden - hidden % 256, hidden % 256))

        def down_step(chunk, carry):
            cols = pl.ds(pl.multiple_of(chunk * width, width), width)
            answer = jnp.dot(hidden_v[...], down_w[:, cols], preferred_element_type=jnp.float32)
            received[mine, :, cols] = answer.reshape(size, CAP, width).astype(jnp.bfloat16)
            return carry

        lax.fori_loop(0, model // width, down_step, 0)
        ship(group, -1, received, answers, moe_send.at[1], back_recv)

        @pl.when(group == 0)
        def _():
            pltpu.make_async_copy(received.at[0], answers.at[0], back_recv.at[0]).start()

        return carry

    lax.fori_loop(0, GROUPS, serve, 0)

    def answered(group, low, count, finish):
        landed(group, answers, back_recv, count)
        lanes = lax.broadcasted_iota(jnp.int32, (positions, count * CAP), 1) + low * CAP
        picks = [
            (lanes == cols_v[:, k : k + 1].astype(jnp.int32)).astype(jnp.float32).astype(jnp.bfloat16)
            for k in range(TOP)
        ]
        for chunk in range(model // width):
            cols = pl.ds(chunk * width, width)
            wide = answers[pl.ds(low, count), :, cols].astype(jnp.float32)
            rows_in = wide.reshape(count * CAP, width).astype(jnp.bfloat16)
            parts = [
                jnp.dot(picks[k], rows_in, preferred_element_type=jnp.float32) * cols_v[:, TOP + k : TOP + k + 1]
                for k in range(TOP)
            ]
            finish(chunk, cols, parts[0] + parts[1])

    def begin(chunk, cols, part):
        total_v[:, cols] = tok_v[:, cols].astype(jnp.float32) + part

    def extend(chunk, cols, part):
        total_v[:, cols] = total_v[:, cols] + part

    puts = []

    def close(chunk, cols, part):
        tok_v[:, cols] = (total_v[:, cols] + part).astype(jnp.bfloat16)
        put = pltpu.make_async_copy(tok_v.at[:, cols], out.at[:, cols], local_sem.at[15 + chunk])
        put.start()
        puts.append(put)

    def combine(group, carry):
        answered(group, group * size, size, extend)
        return carry

    answered(0, 0, size, begin)
    lax.fori_loop(1, GROUPS - 1, combine, 0)
    answered(GROUPS - 1, DEVICES - size, size // 2, extend)
    answered(GROUPS, DEVICES - size // 2, size // 2, close)
    ref = mixed_v.at[pl.ds(0, positions - per)]
    pltpu.make_async_copy(ref, ref, swap_send.at[1]).wait()
    spatial.drained()
    scored.drained()
    valued.drained()
    temporal.drained()
    ref = outgoing.at[pl.ds(0, DEVICES - 1)]
    pltpu.make_async_copy(ref, ref, moe_send.at[0]).wait()
    pltpu.make_async_copy(ref, ref, moe_send.at[1]).wait()
    for put in puts:
        put.wait()


def number_slots(ids_v, gates_v, cols_v, slots_t, loads, clip, tm):
    for load in loads:
        load.wait()
    positions = ids_v.shape[1]
    expert = lax.broadcasted_iota(jnp.int32, (DEVICES, positions), 0)
    e_clip, e_tm = expert // TM, lax.rem(expert, TM)
    dz = lax.rem(e_clip // 2 - clip // 2 + 4, 4)
    dc = lax.rem(lax.rem(e_clip, 2) - lax.rem(clip, 2) + 2, 2)
    dy = lax.rem(e_tm // SIDE - tm // SIDE + 4, 4)
    dx = lax.rem(lax.rem(e_tm, SIDE) - lax.rem(tm, SIDE) + 4, 4)
    order = lax.rem((dz + 4 * dc + 8 * dy + 32 * dx) * INVERSE, DEVICES)
    named = [(ids_v[k : k + 1, :] == expert).astype(jnp.float32) for k in range(TOP)]
    rows = lax.broadcasted_iota(jnp.int32, (positions, positions), 0)
    cols = lax.broadcasted_iota(jnp.int32, (positions, positions), 1)
    before = (rows < cols).astype(jnp.float32).astype(jnp.bfloat16)
    counts = jnp.dot((named[0] + named[1]).astype(jnp.bfloat16), before, preferred_element_type=jnp.float32)
    row = (order * CAP).astype(jnp.float32) + counts
    table = jnp.zeros((DEVICES, positions), jnp.float32)
    for k in range(TOP):
        found = jnp.sum(named[k] * row, axis=0, keepdims=True)
        slots_t[k : k + 1, :] = found.astype(jnp.int32)
        table = jnp.where(expert == k, found, table)
        table = jnp.where(expert == TOP + k, gates_v[k : k + 1, :], table)
    cols_v[...] = table.T


def layer(tokens, sq, sk, sv, sproj, tqkv, tproj, mask, ids, gates, w_gate, w_up, w_down):
    positions, model = tokens.shape
    head_width = sq.shape[1]
    per = positions // TM
    hidden = w_gate.shape[1]
    bf16 = jnp.bfloat16
    vm = lambda *shape: pltpu.VMEM(shape, bf16)
    dma = lambda n: pltpu.SemaphoreType.DMA((n,))
    any_spec = pl.BlockSpec(memory_space=pl.ANY)
    return pl.pallas_call(
        layer_kernel,
        out_shape=jax.ShapeDtypeStruct((positions, model), bf16),
        in_specs=[any_spec] * 13,
        out_specs=any_spec,
        scratch_shapes=[
            vm(positions, model), vm(positions, head_width), vm(positions, model), vm(TM, per, model),
            vm(positions, 3 * head_width), vm(TM, per, head_width),
            pltpu.VMEM((positions, positions), jnp.float32), pltpu.VMEM((TM, TM), jnp.int32),
            pltpu.VMEM((TOP, positions), jnp.int32), pltpu.VMEM((TOP, positions), jnp.float32),
            vm(TM, sproj.shape[0], model), vm(TM, tqkv.shape[0], 3 * head_width), vm(TM, tproj.shape[0], model),
            vm(model, hidden), vm(model, hidden), vm(hidden, model),
            vm(DEVICES, CAP, model), vm(DEVICES, CAP, model), vm(DEVICES, CAP, model),
            vm(positions, hidden), pltpu.VMEM((positions, model), jnp.float32),
            pltpu.VMEM((positions, DEVICES), jnp.float32), pltpu.VMEM((8, positions), jnp.int32),
            pltpu.VMEM((positions, 1), jnp.float32),
            dma(23), dma(4), dma(36), dma(36), dma(36), dma(36), dma(2), dma(5), dma(2), dma(GROUPS), dma(GROUPS + 1),
        ],
        compiler_params=pltpu.CompilerParams(
            collective_id=0, has_side_effects=True, vmem_limit_bytes=67043328
        ),
        name="layer",
    )(tokens, sq, sk, sv, sproj, tqkv, tproj, mask, ids, gates, w_gate, w_up, w_down)


def shards(
    tokens,
    spatial_queries,
    spatial_keys,
    spatial_values,
    spatial_proj,
    temporal_qkv,
    temporal_proj,
    frame_mask,
    expert_ids,
    gate_values,
    expert_gate,
    expert_up,
    expert_down,
):
    positions, model_width = tokens.shape[2:]
    layer_out = layer(
        tokens.reshape(positions, model_width),
        spatial_queries.reshape(positions, -1),
        spatial_keys.reshape(positions, -1),
        spatial_values.reshape(positions, -1),
        spatial_proj,
        temporal_qkv,
        temporal_proj,
        frame_mask.reshape(frame_mask.shape[1:]),
        expert_ids.reshape(positions, TOP).T,
        gate_values.reshape(positions, TOP).T,
        expert_gate[0],
        expert_up[0],
        expert_down[0],
    )
    return layer_out.reshape(tokens.shape)


def solution(mesh):
    placed = (
        P("clip", "tm", None, None),
        P("clip", "tm", None, None),
        P("clip", "tm", None, None),
        P("clip", "tm", None, None),
        P("tm", None),
        P("tm", None),
        P("tm", None),
        P("clip", None, None),
        P("clip", "tm", None, None),
        P("clip", "tm", None, None),
        P(("clip", "tm"), None, None),
        P(("clip", "tm"), None, None),
        P(("clip", "tm"), None, None),
    )
    return jax.shard_map(
        shards, mesh=mesh, in_specs=placed, out_specs=P("clip", "tm", None, None), check_vma=False
    )
```
